32 devices in a mesh: tm: 4 (over y, x), paths: 8 (over z, core).
Axes of the slice: x: 2, y: 2, z: 4, core: 2. Of those that a mesh axis runs over, the one named last changes fastest.
Arguments:
- returns: bfloat16 [128, 4096, 256], P('tm', 'paths'), may hold values from -0.15917969 to 0.15917969
- weights: bfloat16 [256, 64], P('paths'), may hold values from -0.375 to 0.375
Outputs:
- drawdown: float32 [64, 4096], P('tm', 'paths')
The draws below stay inside these ranges and needn't reach their ends.
All inputs are finite; a program needn't handle non-finite values.
Results may differ from the reference program's by a relative error of at most 0.0003.
Values may be sent and summed in bfloat16 or wider, within the bound.
A program may use at most 64 MiB of HBM per device.

```python
import jax
import jax.numpy as jnp
from jax import lax

ASSETS = 256
PORT = 64
T_DEV = 32
STEPS = 128
PATHS = 4096
N_TM = 4


def block_levels(key, shape, shards, smallest, high):
    loudness = 1.0
    for dim, parts in shards:
        heights = jax.random.uniform(jax.random.fold_in(jax.random.fold_in(key, 6), dim), (parts,), jnp.float32, smallest / len(shards), high / len(shards))
        loudness = loudness * jnp.repeat(jnp.exp(heights), shape[dim] // parts).reshape((-1,) + (1,) * (len(shape) - 1 - dim))
    return loudness


def bell_draw(stream_key, dims, spread, limit, split=(), kind=jnp.bfloat16):
    loudness = block_levels(stream_key, dims, split, -0.22, 0.18) if split else 1.0
    array = jax.random.normal(stream_key, dims, jnp.float32) * spread * loudness
    return jnp.minimum(jnp.maximum(array, -limit), limit).astype(kind)


def setup_inputs(seed: int = 0) -> dict:
    keys = jax.random.split(jax.random.key(seed), 3)
    return {
        "returns": bell_draw(keys[0], (STEPS, PATHS, ASSETS), 0.02, 0.15917969, ((0, 4), (1, 8))),
        "weights": bell_draw(keys[1], (ASSETS, PORT), ASSETS ** -0.5, 0.375, ((0, 8),)),
    }


def reference(returns, weights):
    blocks = returns.reshape(N_TM, T_DEV, PATHS, ASSETS)
    holdings = weights.astype(jnp.float32)

    def advance(carry, block):
        level, highest, deepest = carry
        profit = jnp.einsum('tpa,aq->tqp', block.astype(jnp.float32), holdings)
        value = level[None] + jnp.cumsum(profit, axis=0)
        running = jnp.maximum(highest[None], lax.cummax(value, axis=0))
        deepest = jnp.maximum(deepest, jnp.max(running - value, axis=0))
        return (value[-1], running[-1], deepest), None

    zeros = jnp.zeros((PORT, PATHS), jnp.float32)
    final, unused = lax.scan(advance, (zeros, zeros, zeros), blocks)
    return final[2]
```

```python
import functools

import jax
import jax.numpy as jnp
from jax import lax
from jax.experimental import pallas as pl
from jax.experimental.pallas import tpu as pltpu
from jax.sharding import PartitionSpec as P

MESH = pl.DeviceIdType.MESH
CHUNKS = 2
ROWS = 32


def kernel(
    n_tm, n_paths, ret_hbm, w_hbm, out_ref,
    ret, w_ref, wbuf, prof, send, recv, load_sem, own_sem, wsend_sem, wrecv_sem, send_sem, recv_sem,
):
    steps, paths, assets = ret.shape
    ports = w_ref.shape[1]
    block = ports // n_tm
    width = paths // CHUNKS
    half = width // 2
    groups = 1
    tm = lax.axis_index("tm")
    me = lax.axis_index("paths")

    def load(c, g):
        part = (pl.ds(g * steps, steps), pl.ds(c * width, width))
        return pltpu.make_async_copy(ret_hbm.at[part], ret.at[part], load_sem.at[c, g])

    own = pltpu.make_async_copy(w_hbm, w_ref, own_sem)
    own.start()
    for c in range(CHUNKS):
        for g in range(groups):
            load(c, g).start()

    barrier = pltpu.get_barrier_semaphore()
    for d in range(1, n_paths):
        pl.semaphore_signal(
            barrier, inc=1, device_id=(tm, lax.rem(me + d, n_paths)), device_id_type=MESH
        )
    for d in range(1, n_tm):
        pl.semaphore_signal(
            barrier, inc=1, device_id=(lax.rem(tm + d, n_tm), me), device_id_type=MESH
        )
    own.wait()
    pl.semaphore_wait(barrier, n_paths - 1 + n_tm - 1)

    def weight_copy(d):
        return pltpu.make_async_remote_copy(
            src_ref=w_ref,
            dst_ref=wbuf.at[me],
            send_sem=wsend_sem.at[d - 1],
            recv_sem=wrecv_sem.at[d - 1],
            device_id=(tm, lax.rem(me + d, n_paths)),
            device_id_type=MESH,
        )

    def weight_arrival(d):
        return pltpu.make_async_remote_copy(
            src_ref=w_ref,
            dst_ref=wbuf.at[lax.rem(me + n_paths - d, n_paths)],
            send_sem=wsend_sem.at[d - 1],
            recv_sem=wrecv_sem.at[d - 1],
            device_id=(tm, lax.rem(me + d, n_paths)),
            device_id_type=MESH,
        )

    for d in range(1, n_paths):
        weight_copy(d).start()
    wbuf[me] = w_ref[...]
    for d in range(1, n_paths):
        weight_arrival(d).wait_recv()

    held = wbuf[...].reshape(assets, ports)
    blank = jnp.zeros_like(held)
    both = jnp.concatenate(
        [jnp.concatenate([held, blank], axis=1), jnp.concatenate([blank, held], axis=1)], axis=0
    )

    def block_copy(c, d, slot):
        return pltpu.make_async_remote_copy(
            src_ref=send.at[c, lax.rem(tm + d, n_tm)],
            dst_ref=recv.at[c, slot],
            send_sem=send_sem.at[c, d - 1],
            recv_sem=recv_sem.at[c, d - 1],
            device_id=(lax.rem(tm + d, n_tm), me),
            device_id_type=MESH,
        )

    for c in range(CHUNKS):
        first = pl.ds(c * width, half)
        second = pl.ds(c * width + half, half)
        for g in range(groups):
            load(c, g).wait()
            when = pl.ds(g * steps, steps)
            left = ret[when, first, :].reshape(steps * half, assets)
            right = ret[when, second, :].reshape(steps * half, assets)
            prof[c, when] = jnp.dot(
                jnp.concatenate([left, right], axis=1), both, preferred_element_type=jnp.float32
            ).reshape(steps, half, 2 * ports)
        pieces = []
        for r in range(0, half, ROWS):
            value = prof[c, 0, pl.ds(r, ROWS)]
            high, low, fall = value, value, jnp.zeros_like(value)
            for t in range(1, steps):
                value = value + prof[c, t, pl.ds(r, ROWS)]
                high = jnp.maximum(high, value)
                low = jnp.minimum(low, value)
                fall = jnp.maximum(fall, high - value)
            pieces.append((value, high, fall, low))
        for k in range(4):
            whole = jnp.concatenate([piece[k] for piece in pieces], axis=0).T
            for b in range(n_tm):
                rows = b * block
                send[c, b, k, :, 0:half] = whole[rows : rows + block]
                send[c, b, k, :, half:width] = whole[ports + rows : ports + rows + block]
        for d in range(1, n_tm):
            block_copy(c, d, tm).start()
        recv[c, tm] = send[c, tm]

    for c in range(CHUNKS):
        for d in range(1, n_tm):
            block_copy(c, d, lax.rem(tm + n_tm - d, n_tm)).wait_recv()
        level = jnp.zeros((block, width), jnp.float32)
        peak, deepest = level, level
        for s in range(n_tm):
            deepest = jnp.maximum(deepest, recv[c, s, 2])
            deepest = jnp.maximum(deepest, peak - (level + recv[c, s, 3]))
            peak = jnp.maximum(peak, level + recv[c, s, 1])
            level = level + recv[c, s, 0]
        out_ref[:, pl.ds(c * width, width)] = deepest

    for d in range(1, n_paths):
        weight_copy(d).wait_send()
    for c in range(CHUNKS):
        for d in range(1, n_tm):
            block_copy(c, d, tm).wait_send()


def solution(mesh):
    n_tm, n_paths = mesh.shape["tm"], mesh.shape["paths"]

    def shards(returns, weights):
        steps, paths, assets = returns.shape
        share, ports = weights.shape
        block, width = ports // n_tm, paths // CHUNKS
        dma = pltpu.SemaphoreType.DMA
        return pl.pallas_call(
            functools.partial(kernel, n_tm, n_paths),
            out_shape=jax.ShapeDtypeStruct((block, paths), jnp.float32),
            in_specs=[
                pl.BlockSpec(memory_space=pltpu.HBM),
                pl.BlockSpec(memory_space=pltpu.HBM),
            ],
            out_specs=pl.BlockSpec(memory_space=pltpu.VMEM),
            scratch_shapes=[
                pltpu.VMEM((steps, paths, assets), returns.dtype),
                pltpu.VMEM((share, ports), weights.dtype),
                pltpu.VMEM((n_paths, share, ports), weights.dtype),
                pltpu.VMEM((CHUNKS, steps, width // 2, 2 * ports), jnp.float32),
                pltpu.VMEM((CHUNKS, n_tm, 4, block, width), jnp.float32),
                pltpu.VMEM((CHUNKS, n_tm, 4, block, width), jnp.float32),
                dma((CHUNKS, 1)),
                dma,
                dma((n_paths - 1,)),
                dma((n_paths - 1,)),
                dma((CHUNKS, n_tm - 1)),
                dma((CHUNKS, n_tm - 1)),
            ],
            compiler_params=pltpu.CompilerParams(
                collective_id=0, has_side_effects=True, vmem_limit_bytes=32 << 20
            ),
        )(
            pltpu.with_memory_space_constraint(returns, pltpu.HBM),
            pltpu.with_memory_space_constraint(weights, pltpu.HBM),
        )

    in_specs = (P("tm", "paths", None), P("paths", None))
    out_specs = P("tm", "paths")
    return jax.shard_map(shards, mesh=mesh, in_specs=in_specs, out_specs=out_specs, check_vma=False)
```

```python
import functools

import jax
import jax.numpy as jnp
from jax import lax
from jax.experimental import pallas as pl
from jax.experimental.pallas import tpu as pltpu
from jax.sharding import PartitionSpec as P

MESH = pl.DeviceIdType.MESH
CHUNKS = 2
ROWS = 32
LOUD = 64
END, FALL, DIP, LOSS = range(4)
TOP = 2.0**15.75
TINY = 1e-30


def kernel(
    n_tm, n_paths, ret_hbm, w_hbm, out_ref,
    ret, own_w, pair_w, wbuf, part, more, send, recv, loud, louds,
    load_sem, own_sem, wsend_sem, wrecv_sem, send_sem, recv_sem, lsend_sem, lrecv_sem,
):
    steps, paths, assets = ret.shape
    ports = own_w.shape[1]
    block = ports // n_tm
    width = paths // CHUNKS
    half = width // 2
    depth = assets // 2
    subs = half // ROWS
    tm = lax.axis_index("tm")
    me = lax.axis_index("paths")
    near = (2 * me) // n_paths

    barrier = pltpu.get_barrier_semaphore()
    for d in range(1, n_paths):
        pl.semaphore_signal(
            barrier, inc=1, device_id=(tm, lax.rem(me + d, n_paths)), device_id_type=MESH
        )
    for d in range(1, n_tm):
        pl.semaphore_signal(
            barrier, inc=1, device_id=(lax.rem(tm + d, n_tm), me), device_id_type=MESH
        )

    own = pltpu.make_async_copy(w_hbm, own_w, own_sem)
    own.start()

    def load(c):
        rows = pl.ds(c * width, width)
        return pltpu.make_async_copy(ret_hbm.at[:, rows], ret.at[:, rows], load_sem.at[c])

    for c in range(CHUNKS):
        load(c).start()

    own.wait()
    pair_w[...] = jnp.concatenate([own_w[...], own_w[...]], axis=1)
    wbuf[me] = pair_w[...]
    pl.semaphore_wait(barrier, n_paths - 1 + n_tm - 1)

    def weight_copy(d, slot):
        return pltpu.make_async_remote_copy(
            src_ref=pair_w,
            dst_ref=wbuf.at[slot],
            send_sem=wsend_sem.at[d - 1],
            recv_sem=wrecv_sem.at[slot],
            device_id=(tm, lax.rem(me + d, n_paths)),
            device_id_type=MESH,
        )

    for d in range(1, n_paths):
        weight_copy(d, me).start()

    def loud_copy(d, slot):
        return pltpu.make_async_remote_copy(
            src_ref=loud,
            dst_ref=louds.at[slot],
            send_sem=lsend_sem.at[d - 1],
            recv_sem=lrecv_sem.at[d - 1],
            device_id=(lax.rem(tm + d, n_tm), me),
            device_id_type=MESH,
        )

    top = jnp.zeros((LOUD, assets), ret.dtype)
    for c in range(CHUNKS):
        load(c).wait()

        def scan_rows(t, top):
            for r in range(0, width, LOUD):
                top = jnp.maximum(top, jnp.abs(ret[t, pl.ds(c * width + r, LOUD)]))
            return top

        top = lax.fori_loop(0, steps, scan_rows, top)
    loud[...] = jnp.full(loud.shape, jnp.max(top.astype(jnp.float32)), jnp.float32)
    louds[tm] = loud[...]
    for d in range(1, n_tm):
        loud_copy(d, tm).start()

    def side(h):
        held = wbuf[pl.ds(h * (n_paths // 2), n_paths // 2)].reshape(depth, 2 * ports)
        left = lax.broadcasted_iota(jnp.int32, held.shape, 1) < ports
        blank = jnp.zeros_like(held)
        return jnp.concatenate([jnp.where(left, held, blank), jnp.where(left, blank, held)], axis=0)

    def product(c, i, h, both):
        cols = pl.ds(pl.multiple_of(h * depth, depth), depth)
        first = ret[:, pl.ds(c * width + i * ROWS, ROWS), cols].reshape(steps * ROWS, depth)
        second = ret[:, pl.ds(c * width + half + i * ROWS, ROWS), cols].reshape(steps * ROWS, depth)
        return jnp.dot(
            jnp.concatenate([first, second], axis=1), both, preferred_element_type=jnp.float32
        ).reshape(steps, ROWS, 2 * ports)

    def block_copy(c, d, slot):
        return pltpu.make_async_remote_copy(
            src_ref=send.at[c, lax.rem(tm + d, n_tm)],
            dst_ref=recv.at[c, slot],
            send_sem=send_sem.at[c, d - 1],
            recv_sem=recv_sem.at[c, d - 1],
            device_id=(lax.rem(tm + d, n_tm), me),
            device_id_type=MESH,
        )

    group = n_paths // 2
    for k in range(1, group):
        weight_copy(1, near * group + lax.rem(me + k, group)).wait_recv()
    both = side(near)
    for c in range(CHUNKS):
        for i in range(subs):
            part[c, i] = product(c, i, near, both)

    for k in range(group):
        weight_copy(1, (1 - near) * group + k).wait_recv()
    both = side(1 - near)
    for c in range(CHUNKS):
        for i in range(subs):
            more[c, i] = product(c, i, 1 - near, both)
        if c == 0:
            heavy = jnp.max(jnp.abs(wbuf[...].astype(jnp.float32)))
            scale = TOP / jnp.maximum(loud[0:1] * (heavy * (assets * steps)), TINY)
        pieces = []
        for i in range(subs):
            zero = jnp.zeros((ROWS, 2 * ports), jnp.float32)
            end, fall, dip, loss = zero, zero, zero, zero
            for t in range(steps):
                gain = part[c, i, t] + more[c, i, t]
                end = jnp.maximum(end - gain, 0.0)
                fall = jnp.maximum(fall, end)
                loss = loss - gain
                dip = jnp.maximum(dip, loss)
            figures = []
            for k, figure in enumerate((end, fall, dip, loss)):
                code = figure * scale
                code = code * code
                code = code * code
                code = code * code
                if k == LOSS:
                    code = jnp.where(figure < 0, -code, code)
                figures.append(code.astype(jnp.bfloat16))
            pieces.append(figures)
        for k in range(4):
            whole = jnp.concatenate([piece[k] for piece in pieces], axis=0).T
            for b in range(n_tm):
                rows = b * block
                send[c, b, k, :, 0:half] = whole[rows : rows + block]
                send[c, b, k, :, half:width] = whole[ports + rows : ports + rows + block]
        for d in range(1, n_tm):
            block_copy(c, d, tm).start()
        recv[c, tm] = send[c, tm]

    for d in range(1, n_tm):
        loud_copy(d, lax.rem(tm + n_tm - d, n_tm)).wait_recv()
    back = jnp.maximum(louds[:, 0:1] * (heavy * (assets * steps)), TINY) / TOP

    def figure(c, s, k):
        code = recv[c, s, k].astype(jnp.float32)
        size = jnp.exp(jnp.log(jnp.abs(code)) * 0.125) * jnp.tile(back[s], (1, width // back.shape[2]))
        return jnp.where(code < 0, -size, size) if k == LOSS else size

    for c in range(CHUNKS):
        for d in range(1, n_tm):
            block_copy(c, d, lax.rem(tm + n_tm - d, n_tm)).wait_recv()
        end, fall = figure(c, 0, END), figure(c, 0, FALL)
        for s in range(1, n_tm):
            fall = jnp.maximum(jnp.maximum(fall, figure(c, s, FALL)), end + figure(c, s, DIP))
            if s < n_tm - 1:
                end = jnp.maximum(end + figure(c, s, LOSS), figure(c, s, END))
        out_ref[:, pl.ds(c * width, width)] = fall

    for d in range(1, n_paths):
        weight_copy(d, me).wait_send()
    for d in range(1, n_tm):
        loud_copy(d, tm).wait_send()
        for c in range(CHUNKS):
            block_copy(c, d, tm).wait_send()


def solution(mesh):
    n_tm, n_paths = mesh.shape["tm"], mesh.shape["paths"]

    def shards(returns, weights):
        steps, paths, assets = returns.shape
        share, ports = weights.shape
        block, width = ports // n_tm, paths // CHUNKS
        subs = width // 2 // ROWS
        dma = pltpu.SemaphoreType.DMA
        return pl.pallas_call(
            functools.partial(kernel, n_tm, n_paths),
            out_shape=jax.ShapeDtypeStruct((block, paths), jnp.float32),
            in_specs=[
                pl.BlockSpec(memory_space=pltpu.HBM),
                pl.BlockSpec(memory_space=pltpu.HBM),
            ],
            out_specs=pl.BlockSpec(memory_space=pltpu.VMEM),
            scratch_shapes=[
                pltpu.VMEM((steps, paths, assets), returns.dtype),
                pltpu.VMEM((share, ports), weights.dtype),
                pltpu.VMEM((share, 2 * ports), weights.dtype),
                pltpu.VMEM((n_paths, share, 2 * ports), weights.dtype),
                pltpu.VMEM((CHUNKS, subs, steps, ROWS, 2 * ports), jnp.float32),
                pltpu.VMEM((CHUNKS, subs, steps, ROWS, 2 * ports), jnp.float32),
                pltpu.VMEM((CHUNKS, n_tm, 4, block, width), jnp.bfloat16),
                pltpu.VMEM((CHUNKS, n_tm, 4, block, width), jnp.bfloat16),
                pltpu.VMEM((8, 2 * ports), jnp.float32),
                pltpu.VMEM((n_tm, 8, 2 * ports), jnp.float32),
                dma((CHUNKS,)),
                dma,
                dma((n_paths - 1,)),
                dma((n_paths,)),
                dma((CHUNKS, n_tm - 1)),
                dma((CHUNKS, n_tm - 1)),
                dma((n_tm - 1,)),
                dma((n_tm - 1,)),
            ],
            compiler_params=pltpu.CompilerParams(
                collective_id=0, has_side_effects=True, vmem_limit_bytes=32 << 20
            ),
        )(
            pltpu.with_memory_space_constraint(returns, pltpu.HBM),
            pltpu.with_memory_space_constraint(weights, pltpu.HBM),
        )

    in_specs = (P("tm", "paths", None), P("paths", None))
    out_specs = P("tm", "paths")
    return jax.shard_map(shards, mesh=mesh, in_specs=in_specs, out_specs=out_specs, check_vma=False)
```

```python
import functools

import jax
import jax.numpy as jnp
from jax import lax
from jax.experimental import pallas as pl
from jax.experimental.pallas import tpu as pltpu
from jax.sharding import PartitionSpec as P

MESH = pl.DeviceIdType.MESH
CHUNKS = 2
ROWS = 32
LOUD = 32
END, FALL, DIP, LOSS = range(4)
TOP = 2.0**15.75
TINY = 1e-30


def kernel(
    n_tm, n_paths, ret_hbm, w_hbm, out_ref,
    ret, own_w, pair_w, wbuf, part, more, send, recv, loud, louds,
    load_sem, own_sem, ready, near_sem, far_sem, wrecv_sem, send_sem, recv_sem, lsend_sem, lrecv_sem,
):
    steps, paths, assets = ret.shape
    ports = own_w.shape[1]
    block = ports // n_tm
    width = paths // CHUNKS
    half = width // 2
    depth = assets // 2
    subs = half // ROWS
    tm = lax.axis_index("tm")
    me = lax.axis_index("paths")
    share = own_w.shape[0]

    bits = [1 << i for i in range(n_tm.bit_length() - 1)]
    others = range(n_tm - 1, 0, -1)

    def across(k):
        other = tm
        for bit in (b for b in bits if b & k):
            other = other + bit - 2 * bit * ((tm // bit) % 2)
        return other

    half_axis = n_paths // 2
    upper = me // half_axis
    gate = half_axis - 1
    barrier = pltpu.get_barrier_semaphore()

    def greet(t, p):
        pl.semaphore_signal(barrier, inc=1, device_id=(t, p), device_id_type=MESH)

    def fellow(k):
        return upper * half_axis + (me + k) % half_axis

    def greet_upper():
        for p in range(half_axis, n_paths):
            greet(tm, p)

    pl.when(upper == 1)(lambda: greet(tm, gate))
    pl.when(upper == 0)(greet_upper)
    for k in range(1, half_axis):
        greet(tm, fellow(k))
    for k in bits:
        greet(across(k), me)

    own = pltpu.make_async_copy(w_hbm, own_w, own_sem)
    own.start()

    def load(c):
        rows = pl.ds(c * width, width)
        return pltpu.make_async_copy(ret_hbm.at[:, rows], ret.at[:, rows], load_sem.at[c])

    for c in range(CHUNKS):
        load(c).start(priority=1)

    own.wait()
    pair_w[...] = jnp.concatenate([own_w[0 : share // 2], own_w[share // 2 :]], axis=1)
    wbuf[me] = pair_w[...]
    crossing = jnp.logical_or(upper == 1, me == gate).astype(jnp.int32)
    pl.semaphore_wait(barrier, half_axis - 1 + len(bits) + half_axis * crossing)

    for k in (k for k in range(n_tm) if k.bit_count() == 2):
        pl.semaphore_signal(ready.at[k], inc=1, device_id=(across(k & -k), me), device_id_type=MESH)

    def block_of_weights(slot, count, target, sem):
        rows = pl.ds(slot, count)
        return pltpu.make_async_remote_copy(
            src_ref=wbuf.at[rows],
            dst_ref=wbuf.at[rows],
            send_sem=sem,
            recv_sem=wrecv_sem.at[slot],
            device_id=(tm, target),
            device_id_type=MESH,
        )

    def own_weights(target, sem):
        return pltpu.make_async_remote_copy(
            src_ref=pair_w,
            dst_ref=wbuf.at[me],
            send_sem=sem,
            recv_sem=wrecv_sem.at[me],
            device_id=(tm, target),
            device_id_type=MESH,
        )

    def arrival(slot, count):
        block_of_weights(slot, count, me, near_sem.at[0]).wait_recv()

    def send_down(act):
        def down():
            for p in range(half_axis):
                act(own_weights(p, far_sem.at[p]))

        pl.when(upper == 1)(down)

    def send_near(act):
        for k in range(half_axis - 1, 0, -1):
            act(own_weights(fellow(k), near_sem.at[k - 1]))

    def send_over(act):
        def over():
            for p in range(n_paths - 1, half_axis - 1, -1):
                act(block_of_weights(0, half_axis, p, far_sem.at[p - half_axis]))

        pl.when(me == gate)(over)

    def far_arrival():
        def shards():
            for p in range(half_axis, n_paths):
                arrival(p, 1)

        pl.when(upper == 1)(lambda: arrival(0, half_axis))
        pl.when(upper == 0)(shards)

    send_down(lambda copy: copy.start())
    send_near(lambda copy: copy.start())
    for k in range(1, half_axis):
        arrival(fellow(k), 1)
    send_over(lambda copy: copy.start())

    for p in range(2, len(bits) + 1):
        for k in (k for k in range(n_tm) if k.bit_count() == p):
            pl.semaphore_wait(ready.at[k], 1)
        for k in (k for k in range(n_tm) if k.bit_count() == p + 1):
            pl.semaphore_signal(ready.at[k], inc=1, device_id=(across(k & -k), me), device_id_type=MESH)

    def loud_copy(c, k, slot):
        return pltpu.make_async_remote_copy(
            src_ref=loud.at[c],
            dst_ref=louds.at[c, slot],
            send_sem=lsend_sem.at[c, k - 1],
            recv_sem=lrecv_sem.at[c, k - 1],
            device_id=(across(k), me),
            device_id_type=MESH,
        )

    def side(h):
        held = wbuf[pl.ds(h * half_axis, half_axis)]
        swap = jnp.concatenate([held[:, :, ports:], held[:, :, :ports]], axis=2)
        rows = jnp.concatenate([held[:, None], swap[:, None]], axis=1).reshape(depth, 2 * ports)
        spare = jnp.concatenate([swap[:, None], held[:, None]], axis=1).reshape(depth, 2 * ports)
        left = lax.broadcasted_iota(jnp.int32, rows.shape, 1) < ports
        blank = jnp.zeros_like(rows)
        return jnp.concatenate([jnp.where(left, rows, blank), jnp.where(left, blank, spare)], axis=0)

    def product(c, i, h, both):
        cols = pl.ds(pl.multiple_of(h * depth, depth), depth)
        first = ret[:, pl.ds(c * width + i * ROWS, ROWS), cols].reshape(steps * ROWS, depth)
        second = ret[:, pl.ds(c * width + half + i * ROWS, ROWS), cols].reshape(steps * ROWS, depth)
        return jnp.dot(
            jnp.concatenate([first, second], axis=1), both, preferred_element_type=jnp.float32
        ).reshape(steps, ROWS, 2 * ports)

    def block_copy(c, k, slot, first, count):
        figures = pl.ds(first, count)
        return pltpu.make_async_remote_copy(
            src_ref=send.at[c, across(k), figures],
            dst_ref=recv.at[c, slot, figures],
            send_sem=send_sem.at[c, k - 1],
            recv_sem=recv_sem.at[c, k - 1],
            device_id=(across(k), me),
            device_id_type=MESH,
        )

    def by_segment(s, act):
        pl.when(s == 0)(lambda: act(END, 2))
        pl.when(s == n_tm - 1)(lambda: act(FALL, 2))
        pl.when(jnp.logical_and(s > 0, s < n_tm - 1))(lambda: act(END, 4))

    def send_blocks(c, act):
        def blocks(first, count):
            for k in others:
                act(block_copy(c, k, tm, first, count))

        by_segment(tm, blocks)

    def block_arrival(c, k):
        s = across(k)
        by_segment(s, lambda first, count: block_copy(c, k, s, first, count).wait_recv())

    both = side(upper)
    for c in range(CHUNKS):
        load(c).wait()
        for i in range(subs):
            part[c, i] = product(c, i, upper, both)
        top = jnp.zeros((LOUD, assets), ret.dtype)
        for t in range(steps):
            for r in range(c * width, (c + 1) * width, LOUD):
                top = jnp.maximum(top, jnp.abs(ret[t, r : r + LOUD]))
        loud[c] = jnp.full(loud.shape[1:], jnp.max(top.astype(jnp.float32)), jnp.float32)
        for k in others:
            loud_copy(c, k, tm).start()
        louds[c, tm] = loud[c]

    far_arrival()
    both = side(1 - upper)
    for c in range(CHUNKS):
        for i in range(subs):
            more[c, i] = product(c, i, 1 - upper, both)
        if c == 0:
            heavy = jnp.max(jnp.abs(wbuf[...].astype(jnp.float32))) * (assets * steps)
        scale = TOP / jnp.maximum(loud[c, 0:1] * heavy, TINY)
        pieces = []
        for i in range(subs):
            zero = jnp.zeros((ROWS, 2 * ports), jnp.float32)
            end, fall, dip, loss = zero, zero, zero, zero
            for t in range(steps):
                gain = part[c, i, t] + more[c, i, t]
                end = jnp.maximum(end - gain, 0.0)
                fall = jnp.maximum(fall, end)
                loss = loss - gain
                dip = jnp.maximum(dip, loss)
            figures = []
            for k, figure in enumerate((end, fall, dip, loss)):
                code = figure * scale
                code = code * code
                code = code * code
                code = code * code
                if k == LOSS:
                    code = jnp.where(figure < 0, -code, code)
                figures.append(code.astype(jnp.bfloat16))
            pieces.append(figures)
        for k in range(4):
            whole = jnp.concatenate([piece[k] for piece in pieces], axis=0).T
            for b in range(n_tm):
                rows = b * block
                send[c, b, k, :, 0:half] = whole[rows : rows + block]
                send[c, b, k, :, half:width] = whole[ports + rows : ports + rows + block]
        send_blocks(c, lambda copy: copy.start())
        recv[c, tm] = send[c, tm]

    def figure(c, s, k, back):
        code = recv[c, s, k].astype(jnp.float32)
        size = jnp.exp(jnp.log(jnp.abs(code)) * 0.125) * back[s]
        return jnp.where(code < 0, -size, size) if k == LOSS else size

    for c in range(CHUNKS):
        for k in others:
            block_arrival(c, k)
            loud_copy(c, k, across(k)).wait_recv()
        back = jnp.maximum(louds[c, :, 0:1] * heavy, TINY) / TOP
        back = jnp.concatenate([back] * (width // back.shape[2]), axis=2)
        end, fall = figure(c, 0, END, back), figure(c, 0, FALL, back)
        for s in range(1, n_tm):
            fall = jnp.maximum(jnp.maximum(fall, figure(c, s, FALL, back)), end + figure(c, s, DIP, back))
            if s < n_tm - 1:
                end = jnp.maximum(end + figure(c, s, LOSS, back), figure(c, s, END, back))
        out_ref[:, pl.ds(c * width, width)] = fall

    send_down(lambda copy: copy.wait_send())
    send_near(lambda copy: copy.wait_send())
    send_over(lambda copy: copy.wait_send())
    for c in range(CHUNKS):
        for k in others:
            loud_copy(c, k, tm).wait_send()
        send_blocks(c, lambda copy: copy.wait_send())


def solution(mesh):
    n_tm, n_paths = mesh.shape["tm"], mesh.shape["paths"]

    def shards(returns, weights):
        steps, paths, assets = returns.shape
        share, ports = weights.shape
        block, width = ports // n_tm, paths // CHUNKS
        subs = width // 2 // ROWS
        dma = pltpu.SemaphoreType.DMA
        return pl.pallas_call(
            functools.partial(kernel, n_tm, n_paths),
            out_shape=jax.ShapeDtypeStruct((block, paths), jnp.float32),
            in_specs=[
                pl.BlockSpec(memory_space=pltpu.HBM),
                pl.BlockSpec(memory_space=pltpu.HBM),
            ],
            out_specs=pl.BlockSpec(memory_space=pltpu.VMEM),
            scratch_shapes=[
                pltpu.VMEM((steps, paths, assets), returns.dtype),
                pltpu.VMEM((share, ports), weights.dtype),
                pltpu.VMEM((share // 2, 2 * ports), weights.dtype),
                pltpu.VMEM((n_paths, share // 2, 2 * ports), weights.dtype),
                pltpu.VMEM((CHUNKS, subs, steps, ROWS, 2 * ports), jnp.float32),
                pltpu.VMEM((CHUNKS, subs, steps, ROWS, 2 * ports), jnp.float32),
                pltpu.VMEM((CHUNKS, n_tm, 4, block, width), jnp.bfloat16),
                pltpu.VMEM((CHUNKS, n_tm, 4, block, width), jnp.bfloat16),
                pltpu.VMEM((CHUNKS, 8, 2 * ports), jnp.float32),
                pltpu.VMEM((CHUNKS, n_tm, 8, 2 * ports), jnp.float32),
                dma((CHUNKS,)),
                dma,
                pltpu.SemaphoreType.REGULAR((n_tm,)),
                dma((n_paths // 2 - 1,)),
                dma((n_paths // 2,)),
                dma((n_paths,)),
                dma((CHUNKS, n_tm - 1)),
                dma((CHUNKS, n_tm - 1)),
                dma((CHUNKS, n_tm - 1)),
                dma((CHUNKS, n_tm - 1)),
            ],
            compiler_params=pltpu.CompilerParams(
                collective_id=0, has_side_effects=True, vmem_limit_bytes=32 << 20
            ),
        )(
            pltpu.with_memory_space_constraint(returns, pltpu.HBM),
            pltpu.with_memory_space_constraint(weights, pltpu.HBM),
        )

    in_specs = (P("tm", "paths", None), P("paths", None))
    out_specs = P("tm", "paths")
    return jax.shard_map(shards, mesh=mesh, in_specs=in_specs, out_specs=out_specs, check_vma=False)
```

```python
import functools

import jax
import jax.numpy as jnp
from jax import lax
from jax.experimental import pallas as pl
from jax.experimental.pallas import tpu as pltpu
from jax.sharding import PartitionSpec as P

MESH = pl.DeviceIdType.MESH
CHUNKS = 2
ROWS = 32
PIECES = 8
AHEAD = 8
LOUD = 64
END, FALL, DIP, LOSS = range(4)
TOP = 2.0**15.75
TINY = 1e-30


def kernel(
    n_tm, n_paths, ret_hbm, w_hbm, out_ref,
    ret, own_w, pair_w, wbuf, part, more, send, recv, loud, louds, values,
    load_sem, own_sem, ready, opened, near_sem, far_sem, wrecv_sem, send_sem, recv_sem, lsend_sem, lrecv_sem,
):
    steps, paths, assets = ret.shape
    ports = own_w.shape[1]
    block = ports // n_tm
    width = paths // CHUNKS
    half = width // 2
    depth = assets // 2
    subs = half // ROWS
    tm = lax.axis_index("tm")
    me = lax.axis_index("paths")
    share = own_w.shape[0]

    bits = [1 << i for i in range(n_tm.bit_length() - 1)]
    others = sorted(range(1, n_tm), key=lambda k: -k.bit_count())
    arrivals = others[::-1]

    def across(k):
        other = tm
        for bit in (b for b in bits if b & k):
            other = other + bit - 2 * bit * ((tm // bit) % 2)
        return other

    half_axis = n_paths // 2
    upper = me // half_axis
    gate = half_axis - 1
    barrier = pltpu.get_barrier_semaphore()

    def greet(t, p):
        pl.semaphore_signal(barrier, inc=1, device_id=(t, p), device_id_type=MESH)

    def fellow(k):
        return upper * half_axis + (me + k) % half_axis

    def greet_upper():
        for p in range(half_axis, n_paths):
            greet(tm, p)

    pl.when(upper == 1)(lambda: greet(tm, gate))
    pl.when(upper == 0)(greet_upper)
    for k in range(1, half_axis):
        pl.when(fellow(k) != gate)(lambda: greet(tm, fellow(k)))
    for k in bits:
        greet(across(k), me)

    own = pltpu.make_async_copy(w_hbm, own_w, own_sem)
    own.start()

    def load(c):
        days = pl.ds(c * (steps // PIECES), steps // PIECES)
        return pltpu.make_async_copy(ret_hbm.at[days], ret.at[days], load_sem.at[c])

    for c in range(AHEAD):
        load(c).start(priority=1)

    own.wait()
    pair_w[...] = jnp.concatenate([own_w[0 : share // 2], own_w[share // 2 :]], axis=1)
    wbuf[me] = pair_w[...]
    pl.when(me != gate)(lambda: pl.semaphore_wait(barrier, half_axis - 1 + len(bits) + half_axis * upper))

    def open_gate():
        pl.semaphore_signal(opened, inc=1, device_id=(tm, gate), device_id_type=MESH)

    pl.when(jnp.logical_and(upper == 0, me != gate))(open_gate)
    pl.when(me == gate)(lambda: pl.semaphore_wait(opened, half_axis - 1))

    def block_of_weights(slot, count, target, sem):
        rows = pl.ds(slot, count)
        return pltpu.make_async_remote_copy(
            src_ref=wbuf.at[rows],
            dst_ref=wbuf.at[rows],
            send_sem=sem,
            recv_sem=wrecv_sem.at[slot],
            device_id=(tm, target),
            device_id_type=MESH,
        )

    def own_weights(target, sem):
        return pltpu.make_async_remote_copy(
            src_ref=pair_w,
            dst_ref=wbuf.at[me],
            send_sem=sem,
            recv_sem=wrecv_sem.at[me],
            device_id=(tm, target),
            device_id_type=MESH,
        )

    def arrival(slot, count):
        block_of_weights(slot, count, me, near_sem.at[0]).wait_recv()

    def send_down(act):
        def down():
            for p in range(half_axis):
                act(own_weights(p, far_sem.at[p]))

        pl.when(upper == 1)(down)

    def send_near(act):
        for k in range(half_axis - 1, 0, -1):
            act(own_weights(fellow(k), near_sem.at[k - 1]))

    def send_over(act):
        def over():
            for p in range(n_paths - 1, half_axis - 1, -1):
                act(block_of_weights(0, half_axis, p, far_sem.at[p - half_axis]))

        pl.when(me == gate)(over)

    def far_arrival():
        def shards():
            for p in range(half_axis, n_paths):
                arrival(p, 1)

        pl.when(upper == 1)(lambda: arrival(0, half_axis))
        pl.when(upper == 0)(shards)

    send_down(lambda copy: copy.start())
    send_near(lambda copy: copy.start())
    pl.when(me == gate)(lambda: pl.semaphore_wait(barrier, half_axis + len(bits)))

    for k in (k for k in range(n_tm) if k.bit_count() == 2):
        pl.semaphore_signal(ready.at[k], inc=1, device_id=(across(k & -k), me), device_id_type=MESH)

    def near_arrival():
        for k in range(1, half_axis):
            arrival(fellow(k), 1)

    pl.when(me == gate)(near_arrival)
    send_over(lambda copy: copy.start())

    for p in range(2, len(bits) + 1):
        for k in (k for k in range(n_tm) if k.bit_count() == p):
            pl.semaphore_wait(ready.at[k], 1)
        for k in (k for k in range(n_tm) if k.bit_count() == p + 1):
            pl.semaphore_signal(ready.at[k], inc=1, device_id=(across(k & -k), me), device_id_type=MESH)

    def loud_copy(k, slot):
        return pltpu.make_async_remote_copy(
            src_ref=loud,
            dst_ref=louds.at[slot],
            send_sem=lsend_sem.at[k - 1],
            recv_sem=lrecv_sem.at[k - 1],
            device_id=(across(k), me),
            device_id_type=MESH,
        )

    top = jnp.zeros((LOUD, assets), ret.dtype)
    for c in range(PIECES):
        load(c).wait()
        if c + AHEAD < PIECES:
            load(c + AHEAD).start(priority=1)

        def look(i, top):
            t, r = c * (steps // PIECES) + i // (paths // (4 * LOUD)), i % (paths // (4 * LOUD)) * (4 * LOUD)
            for q in range(4):
                top = jnp.maximum(top, jnp.abs(ret[t, pl.ds(r + q * LOUD, LOUD)]))
            return top

        top = lax.fori_loop(0, steps // PIECES * (paths // (4 * LOUD)), look, top)
    loud[...] = jnp.full(loud.shape, jnp.max(top.astype(jnp.float32)), jnp.float32)
    for k in others:
        loud_copy(k, tm).start()
    louds[tm] = loud[...]
    pl.when(me != gate)(near_arrival)

    def side(h):
        held = wbuf[pl.ds(h * half_axis, half_axis)]
        swap = jnp.concatenate([held[:, :, ports:], held[:, :, :ports]], axis=2)
        rows = jnp.concatenate([held[:, None], swap[:, None]], axis=1).reshape(depth, 2 * ports)
        spare = jnp.concatenate([swap[:, None], held[:, None]], axis=1).reshape(depth, 2 * ports)
        left = lax.broadcasted_iota(jnp.int32, rows.shape, 1) < ports
        blank = jnp.zeros_like(rows)
        return jnp.concatenate([jnp.where(left, rows, blank), jnp.where(left, blank, spare)], axis=0)

    def product(c, i, h, both):
        cols = pl.ds(pl.multiple_of(h * depth, depth), depth)
        first = ret[:, pl.ds(c * width + i * ROWS, ROWS), cols].reshape(steps * ROWS, depth)
        second = ret[:, pl.ds(c * width + half + i * ROWS, ROWS), cols].reshape(steps * ROWS, depth)
        return jnp.dot(
            jnp.concatenate([first, second], axis=1), both, preferred_element_type=jnp.float32
        ).reshape(steps, ROWS, 2 * ports)

    def block_copy(c, k, slot, first, count):
        figures = pl.ds(first, count)
        return pltpu.make_async_remote_copy(
            src_ref=send.at[c, across(k), figures],
            dst_ref=recv.at[c, slot, figures],
            send_sem=send_sem.at[c, k - 1],
            recv_sem=recv_sem.at[c, k - 1],
            device_id=(across(k), me),
            device_id_type=MESH,
        )

    def by_segment(s, act):
        pl.when(s == 0)(lambda: act(END, 2))
        pl.when(s == n_tm - 1)(lambda: act(FALL, 2))
        pl.when(jnp.logical_and(s > 0, s < n_tm - 1))(lambda: act(END, 4))

    def send_blocks(c, act, late):
        def blocks(first, count):
            for k in others:
                if k.bit_count() > 1:
                    pl.when((across(k) > 0) == late)(lambda: act(block_copy(c, k, tm, first, count)))
                elif not late:
                    act(block_copy(c, k, tm, first, count))

        by_segment(tm, blocks)

    def block_arrival(c, k):
        s = across(k)
        by_segment(s, lambda first, count: block_copy(c, k, s, first, count).wait_recv())

    both = side(upper)
    for c in range(CHUNKS):
        for i in range(subs):
            part[c, i] = product(c, i, upper, both)

    far_arrival()
    both = side(1 - upper)
    for c in range(CHUNKS):
        for i in range(subs):
            more[c, i] = product(c, i, 1 - upper, both)
        if c == 0:
            heavy = jnp.max(jnp.abs(wbuf[...].astype(jnp.float32))) * (assets * steps)
        scale = TOP / jnp.maximum(loud[0:1] * heavy, TINY)
        pieces = []
        for i in range(subs):
            zero = jnp.zeros((ROWS, 2 * ports), jnp.float32)
            end, fall, dip, loss = zero, zero, zero, zero
            for t in range(steps):
                gain = part[c, i, t] + more[c, i, t]
                end = jnp.maximum(end - gain, 0.0)
                fall = jnp.maximum(fall, end)
                loss = loss - gain
                dip = jnp.maximum(dip, loss)
            figures = []
            for k, figure in enumerate((end, fall, dip, loss)):
                code = figure * scale
                code = code * code
                code = code * code
                code = code * code
                if k == LOSS:
                    code = jnp.where(figure < 0, -code, code)
                figures.append(code.astype(jnp.bfloat16))
            pieces.append(figures)
        for k in range(4):
            whole = jnp.concatenate([piece[k] for piece in pieces], axis=0).T
            for b in range(n_tm):
                rows = b * block
                send[c, b, k, :, 0:half] = whole[rows : rows + block]
                send[c, b, k, :, half:width] = whole[ports + rows : ports + rows + block]
        send_blocks(c, lambda copy: copy.start(), False)

    for c in range(CHUNKS):
        send_blocks(c, lambda copy: copy.start(), True)
    send_down(lambda copy: copy.wait_send())
    send_near(lambda copy: copy.wait_send())
    send_over(lambda copy: copy.wait_send())
    for k in others:
        loud_copy(k, tm).wait_send()
        loud_copy(k, across(k)).wait_recv()

    def decode(codes, s):
        unit = jnp.maximum(louds[s, 0:1] * heavy, TINY) / TOP
        unit = jnp.concatenate([unit] * (width // unit.shape[1]), axis=1)
        code = codes.astype(jnp.float32)
        size = jnp.exp(jnp.log(jnp.abs(code)) * 0.125) * unit[None]
        values[s] = jnp.concatenate([size[:LOSS], jnp.where(code[LOSS:] < 0, -size[LOSS:], size[LOSS:])], axis=0)

    for c in range(CHUNKS):
        decode(send[c, tm], tm)
        for k in arrivals:
            block_arrival(c, k)
            decode(recv[c, across(k)], across(k))
        end, fall = values[0, END], values[0, FALL]
        for s in range(1, n_tm):
            fall = jnp.maximum(jnp.maximum(fall, values[s, FALL]), end + values[s, DIP])
            if s < n_tm - 1:
                end = jnp.maximum(end + values[s, LOSS], values[s, END])
        out_ref[:, pl.ds(c * width, width)] = fall

    for c in range(CHUNKS):
        for late in (False, True):
            send_blocks(c, lambda copy: copy.wait_send(), late)


def solution(mesh):
    n_tm, n_paths = mesh.shape["tm"], mesh.shape["paths"]

    def shards(returns, weights):
        steps, paths, assets = returns.shape
        share, ports = weights.shape
        block, width = ports // n_tm, paths // CHUNKS
        subs = width // 2 // ROWS
        dma = pltpu.SemaphoreType.DMA
        return pl.pallas_call(
            functools.partial(kernel, n_tm, n_paths),
            out_shape=jax.ShapeDtypeStruct((block, paths), jnp.float32),
            in_specs=[
                pl.BlockSpec(memory_space=pltpu.HBM),
                pl.BlockSpec(memory_space=pltpu.HBM),
            ],
            out_specs=pl.BlockSpec(memory_space=pltpu.VMEM),
            scratch_shapes=[
                pltpu.VMEM((steps, paths, assets), returns.dtype),
                pltpu.VMEM((share, ports), weights.dtype),
                pltpu.VMEM((share // 2, 2 * ports), weights.dtype),
                pltpu.VMEM((n_paths, share // 2, 2 * ports), weights.dtype),
                pltpu.VMEM((CHUNKS, subs, steps, ROWS, 2 * ports), jnp.float32),
                pltpu.VMEM((CHUNKS, subs, steps, ROWS, 2 * ports), jnp.float32),
                pltpu.VMEM((CHUNKS, n_tm, 4, block, width), jnp.bfloat16),
                pltpu.VMEM((CHUNKS, n_tm, 4, block, width), jnp.bfloat16),
                pltpu.VMEM((8, 2 * ports), jnp.float32),
                pltpu.VMEM((n_tm, 8, 2 * ports), jnp.float32),
                pltpu.VMEM((n_tm, 4, block, width), jnp.float32),
                dma((PIECES,)),
                dma,
                pltpu.SemaphoreType.REGULAR((n_tm,)),
                pltpu.SemaphoreType.REGULAR,
                dma((n_paths // 2 - 1,)),
                dma((n_paths // 2,)),
                dma((n_paths,)),
                dma((CHUNKS, n_tm - 1)),
                dma((CHUNKS, n_tm - 1)),
                dma((n_tm - 1,)),
                dma((n_tm - 1,)),
            ],
            compiler_params=pltpu.CompilerParams(
                collective_id=0, has_side_effects=True, vmem_limit_bytes=32 << 20
            ),
        )(
            pltpu.with_memory_space_constraint(returns, pltpu.HBM),
            pltpu.with_memory_space_constraint(weights, pltpu.HBM),
        )

    in_specs = (P("tm", "paths", None), P("paths", None))
    out_specs = P("tm", "paths")
    return jax.shard_map(shards, mesh=mesh, in_specs=in_specs, out_specs=out_specs, check_vma=False)
```

```python
import functools

import jax
import jax.numpy as jnp
from jax import lax
from jax.experimental import pallas as pl
from jax.experimental.pallas import tpu as pltpu
from jax.sharding import PartitionSpec as P

MESH = pl.DeviceIdType.MESH
CHUNKS = 2
ROWS = 32
PIECES = 4
LOUD = 64
END, FALL, DIP, LOSS = range(4)
TOP = 2.0**15.75
TINY = 1e-30


def kernel(
    n_tm, n_paths, ret_hbm, w_hbm, out_ref,
    ret, own_w, pair_w, wbuf, part, more, send, recv, loud, louds, values,
    load_sem, own_sem, ready, opened, near_sem, near_recv_sem, far_sem, far_recv_sem, send_sem, recv_sem, lsend_sem, lrecv_sem,
):
    steps, paths, assets = ret.shape
    ports = own_w.shape[1]
    block = ports // n_tm
    width = paths // CHUNKS
    half = width // 2
    depth = assets // 2
    subs = half // ROWS
    tm = lax.axis_index("tm")
    me = lax.axis_index("paths")
    share = own_w.shape[0]

    own = pltpu.make_async_copy(w_hbm, own_w, own_sem)
    own.start()
    bits = [1 << i for i in range(n_tm.bit_length() - 1)]
    others = sorted(range(1, n_tm), key=lambda k: -k.bit_count())
    arrivals = others[::-1]
    apart = [k for k in others if k.bit_count() > 1]

    def across(k):
        other = tm
        for bit in (b for b in bits if b & k):
            other = other + bit - 2 * bit * ((tm // bit) % 2)
        return other

    half_axis = n_paths // 2
    upper = me // half_axis
    gate = half_axis - 1
    barrier = pltpu.get_barrier_semaphore()

    def greet(t, p):
        pl.semaphore_signal(barrier, inc=1, device_id=(t, p), device_id_type=MESH)

    def fellow(k):
        return upper * half_axis + (me + k) % half_axis

    def greet_upper():
        for p in range(half_axis, n_paths):
            greet(tm, p)

    pl.when(upper == 1)(lambda: greet(tm, gate))
    pl.when(upper == 0)(greet_upper)
    for k in range(1, half_axis):
        pl.when(fellow(k) != gate)(lambda: greet(tm, fellow(k)))
    for k in bits:
        greet(across(k), me)


    def load(c):
        days = pl.ds(c * (steps // PIECES), steps // PIECES)
        return pltpu.make_async_copy(ret_hbm.at[days], ret.at[days], load_sem.at[c])

    for c in range(PIECES):
        load(c).start(priority=1)

    own.wait()
    pair_w[...] = jnp.concatenate([own_w[0 : share // 2], own_w[share // 2 :]], axis=1)
    wbuf[me] = pair_w[...]
    pl.when(me != gate)(lambda: pl.semaphore_wait(barrier, half_axis - 1 + len(bits) + half_axis * upper))

    def open_gate():
        pl.semaphore_signal(opened, inc=1, device_id=(tm, gate), device_id_type=MESH)

    pl.when(jnp.logical_and(upper == 0, me != gate))(open_gate)
    pl.when(me == gate)(lambda: pl.semaphore_wait(opened, half_axis - 1))

    def weights_copy(source, rows, target, sems):
        return pltpu.make_async_remote_copy(
            src_ref=source,
            dst_ref=wbuf.at[rows],
            send_sem=sems[0],
            recv_sem=sems[1],
            device_id=(tm, target),
            device_id_type=MESH,
        )

    def weights_wait(count, sems):
        rows = pl.ds(0, count)
        return weights_copy(wbuf.at[rows], rows, gate, sems)

    near_sems = near_sem, near_recv_sem

    def far_sems(p):
        return far_sem.at[p], far_recv_sem

    def send_down(act):
        def down():
            for p in range(half_axis):
                act(weights_copy(pair_w, me, p, far_sems(p)))

        pl.when(upper == 1)(down)

    def send_near(act):
        for k in range(half_axis - 1, 0, -1):
            act(weights_copy(pair_w, me, fellow(k), near_sems))

    def send_over(act):
        rows = pl.ds(0, half_axis)

        def over():
            for p in range(half_axis - 1, -1, -1):
                act(weights_copy(wbuf.at[rows], rows, half_axis + p, far_sems(p)))

        pl.when(me == gate)(over)

    send_down(lambda copy: copy.start())
    send_near(lambda copy: copy.start())
    pl.when(me == gate)(lambda: pl.semaphore_wait(barrier, half_axis + len(bits)))

    for k in (k for k in range(n_tm) if k.bit_count() == 2):
        pl.semaphore_signal(ready.at[apart.index(k)], inc=1, device_id=(across(k & -k), me), device_id_type=MESH)

    def near_arrival():
        weights_wait(half_axis - 1, near_sems).wait_recv()

    pl.when(me == gate)(near_arrival)
    send_over(lambda copy: copy.start())

    for p in range(2, len(bits) + 1):
        for k in (k for k in range(n_tm) if k.bit_count() == p):
            pl.semaphore_wait(ready.at[apart.index(k)], 1)
        for k in (k for k in range(n_tm) if k.bit_count() == p + 1):
            pl.semaphore_signal(ready.at[apart.index(k)], inc=1, device_id=(across(k & -k), me), device_id_type=MESH)

    def loud_copy(k, source, slot):
        return pltpu.make_async_remote_copy(
            src_ref=source,
            dst_ref=louds.at[slot],
            send_sem=lsend_sem,
            recv_sem=lrecv_sem,
            device_id=(across(k), me),
            device_id_type=MESH,
        )

    top = jnp.zeros((LOUD, assets), ret.dtype)
    for c in range(PIECES):
        load(c).wait()

        def look(i, top):
            t, r = c * (steps // PIECES) + i // (paths // (4 * LOUD)), i % (paths // (4 * LOUD)) * (4 * LOUD)
            for q in range(4):
                top = jnp.maximum(top, jnp.abs(ret[t, pl.ds(r + q * LOUD, LOUD)]))
            return top

        top = lax.fori_loop(0, steps // PIECES * (paths // (4 * LOUD)), look, top)
    loud[...] = jnp.full(loud.shape, jnp.max(top.astype(jnp.float32)), jnp.float32)
    for k in others:
        loud_copy(k, loud, tm).start()
    louds[tm] = loud[...]
    pl.when(me != gate)(near_arrival)

    def side(h):
        held = wbuf[pl.ds(h * half_axis, half_axis)]
        swap = jnp.concatenate([held[:, :, ports:], held[:, :, :ports]], axis=2)
        rows = jnp.concatenate([held[:, None], swap[:, None]], axis=1).reshape(depth, 2 * ports)
        spare = jnp.concatenate([swap[:, None], held[:, None]], axis=1).reshape(depth, 2 * ports)
        left = lax.broadcasted_iota(jnp.int32, rows.shape, 1) < ports
        blank = jnp.zeros_like(rows)
        return jnp.concatenate([jnp.where(left, rows, blank), jnp.where(left, blank, spare)], axis=0)

    def product(c, i, h, both):
        cols = pl.ds(pl.multiple_of(h * depth, depth), depth)
        first = ret[:, pl.ds(c * width + i * ROWS, ROWS), cols].reshape(steps * ROWS, depth)
        second = ret[:, pl.ds(c * width + half + i * ROWS, ROWS), cols].reshape(steps * ROWS, depth)
        return jnp.dot(
            jnp.concatenate([first, second], axis=1), both, preferred_element_type=jnp.float32
        ).reshape(steps, ROWS, 2 * ports)

    def block_copy(c, k, target, slot, first, count):
        figures = pl.ds(first, count)
        return pltpu.make_async_remote_copy(
            src_ref=send.at[c, target, figures],
            dst_ref=recv.at[c, slot, figures],
            send_sem=send_sem,
            recv_sem=recv_sem.at[c, k - 1] if isinstance(c, int) else recv_sem.at[0, 0],
            device_id=(across(k), me),
            device_id_type=MESH,
        )

    def by_segment(s, act):
        pl.when(s == 0)(lambda: act(END, 2))
        pl.when(s == n_tm - 1)(lambda: act(FALL, 2))
        pl.when(jnp.logical_and(s > 0, s < n_tm - 1))(lambda: act(END, 4))

    def send_blocks(c, act, late):
        def blocks(first, count):
            for k in others:
                if k.bit_count() > 1:
                    pl.when((across(k) > 0) == late)(lambda: act(block_copy(c, k, across(k), tm, first, count)))
                elif not late:
                    act(block_copy(c, k, across(k), tm, first, count))

        by_segment(tm, blocks)

    def block_arrival(c, k):
        s = across(k)
        by_segment(s, lambda first, count: block_copy(c, k, s, s, first, count).wait_recv())

    both = side(upper)
    for c in range(CHUNKS):
        for i in range(subs):
            part[c, i] = product(c, i, upper, both)

    weights_wait(half_axis, far_sems(0)).wait_recv()
    both = side(1 - upper)
    for c in range(CHUNKS):
        for i in range(subs):
            more[c, i] = product(c, i, 1 - upper, both)
        if c == 0:
            heavy = jnp.max(jnp.abs(wbuf[...].astype(jnp.float32))) * (assets * steps)
        scale = TOP / jnp.maximum(loud[0:1] * heavy, TINY)
        pieces = []
        for i in range(subs):
            zero = jnp.zeros((ROWS, 2 * ports), jnp.float32)
            end, fall, dip, loss = zero, zero, zero, zero
            for t in range(steps):
                gain = part[c, i, t] + more[c, i, t]
                end = jnp.maximum(end - gain, 0.0)
                fall = jnp.maximum(fall, end)
                loss = loss - gain
                dip = jnp.maximum(dip, loss)
            figures = []
            for k, figure in enumerate((end, fall, dip, loss)):
                code = figure * scale
                code = code * code
                code = code * code
                code = code * code
                if k == LOSS:
                    code = jnp.where(figure < 0, -code, code)
                figures.append(code.astype(jnp.bfloat16))
            pieces.append(figures)
        for k in range(4):
            whole = jnp.concatenate([piece[k] for piece in pieces], axis=0).T
            for b in range(n_tm):
                rows = b * block
                send[c, b, k, :, 0:half] = whole[rows : rows + block]
                send[c, b, k, :, half:width] = whole[ports + rows : ports + rows + block]
        send_blocks(c, lambda copy: copy.start(), False)

    for c in range(CHUNKS):
        send_blocks(c, lambda copy: copy.start(), True)
    send_down(lambda copy: copy.wait_send())
    weights_wait(half_axis - 1, near_sems).wait_send()
    send_over(lambda copy: copy.wait_send())
    rest = pl.ds(0, n_tm - 1)
    loud_copy(1, louds.at[rest], rest).wait_send()
    loud_copy(1, louds.at[rest], rest).wait_recv()

    def decode(codes, s):
        unit = jnp.maximum(louds[s, 0:1] * heavy, TINY) / TOP
        unit = jnp.concatenate([unit] * (width // unit.shape[1]), axis=1)
        code = codes.astype(jnp.float32)
        size = jnp.exp(jnp.log(jnp.abs(code)) * 0.125) * unit[None]
        values[s] = jnp.concatenate([size[:LOSS], jnp.where(code[LOSS:] < 0, -size[LOSS:], size[LOSS:])], axis=0)

    def drain(first, count):
        block_copy(pl.ds(0, CHUNKS), 1, rest, rest, first, count).wait_send()

    for c in range(CHUNKS):
        decode(send[c, tm], tm)
        for k in arrivals:
            if (c, k) == (CHUNKS - 1, arrivals[-1]):
                by_segment(tm, drain)
            block_arrival(c, k)
            decode(recv[c, across(k)], across(k))
        end, fall = values[0, END], values[0, FALL]
        for s in range(1, n_tm):
            fall = jnp.maximum(jnp.maximum(fall, values[s, FALL]), end + values[s, DIP])
            if s < n_tm - 1:
                end = jnp.maximum(end + values[s, LOSS], values[s, END])
        out_ref[:, pl.ds(c * width, width)] = fall


def solution(mesh):
    n_tm, n_paths = mesh.shape["tm"], mesh.shape["paths"]

    def shards(returns, weights):
        steps, paths, assets = returns.shape
        share, ports = weights.shape
        block, width = ports // n_tm, paths // CHUNKS
        subs = width // 2 // ROWS
        dma = pltpu.SemaphoreType.DMA
        return pl.pallas_call(
            functools.partial(kernel, n_tm, n_paths),
            out_shape=jax.ShapeDtypeStruct((block, paths), jnp.float32),
            in_specs=[
                pl.BlockSpec(memory_space=pltpu.HBM),
                pl.BlockSpec(memory_space=pltpu.HBM),
            ],
            out_specs=pl.BlockSpec(memory_space=pltpu.VMEM),
            scratch_shapes=[
                pltpu.VMEM((steps, paths, assets), returns.dtype),
                pltpu.VMEM((share, ports), weights.dtype),
                pltpu.VMEM((share // 2, 2 * ports), weights.dtype),
                pltpu.VMEM((n_paths, share // 2, 2 * ports), weights.dtype),
                pltpu.VMEM((CHUNKS, subs, steps, ROWS, 2 * ports), jnp.float32),
                pltpu.VMEM((CHUNKS, subs, steps, ROWS, 2 * ports), jnp.float32),
                pltpu.VMEM((CHUNKS, n_tm, 4, block, width), jnp.bfloat16),
                pltpu.VMEM((CHUNKS, n_tm, 4, block, width), jnp.bfloat16),
                pltpu.VMEM((8, 2 * ports), jnp.float32),
                pltpu.VMEM((n_tm, 8, 2 * ports), jnp.float32),
                pltpu.VMEM((n_tm, 4, block, width), jnp.float32),
                dma((PIECES,)),
                dma,
                pltpu.SemaphoreType.REGULAR((n_tm - n_tm.bit_length(),)),
                pltpu.SemaphoreType.REGULAR,
                dma,
                dma,
                dma((n_paths // 2,)),
                dma,
                dma,
                dma((CHUNKS, n_tm - 1)),
                dma,
                dma,
            ],
            compiler_params=pltpu.CompilerParams(
                collective_id=0, has_side_effects=True, vmem_limit_bytes=32 << 20
            ),
        )(
            pltpu.with_memory_space_constraint(returns, pltpu.HBM),
            pltpu.with_memory_space_constraint(weights, pltpu.HBM),
        )

    in_specs = (P("tm", "paths", None), P("paths", None))
    out_specs = P("tm", "paths")
    return jax.shard_map(shards, mesh=mesh, in_specs=in_specs, out_specs=out_specs, check_vma=False)
```

```python
import functools

import jax
import jax.numpy as jnp
from jax import lax
from jax.experimental import pallas as pl
from jax.experimental.pallas import tpu as pltpu
from jax.sharding import PartitionSpec as P

MESH = pl.DeviceIdType.MESH
CHUNKS = 2
ROWS = 32
PIECES = 4
LOUD = 64
END, FALL, DIP, LOSS = range(4)
TOP = 2.0**15.75
TINY = 1e-30


def kernel(
    n_tm, n_paths, ret_hbm, w_hbm, out_ref,
    ret, own_w, pair_w, wbuf, part, more, send, recv, loud, louds, values,
    load_sem, own_sem, told, opened, near_sem, near_recv_sem, far_sem, far_recv_sem, send_sem, recv_sem, lsend_sem, lrecv_sem,
):
    steps, paths, assets = ret.shape
    ports = own_w.shape[1]
    block = ports // n_tm
    width = paths // CHUNKS
    half = width // 2
    depth = assets // 2
    subs = half // ROWS
    tm = lax.axis_index("tm")
    me = lax.axis_index("paths")
    share = own_w.shape[0]

    own = pltpu.make_async_copy(w_hbm, own_w, own_sem)
    own.start()
    bits = [1 << i for i in range(n_tm.bit_length() - 1)]
    others = sorted(range(1, n_tm), key=lambda k: -k.bit_count())
    arrivals = others[::-1]

    def across(k):
        other = tm
        for bit in (b for b in bits if b & k):
            other = other + bit - 2 * bit * ((tm // bit) % 2)
        return other

    half_axis = n_paths // 2
    upper = me // half_axis
    gate = half_axis - 1
    barrier = pltpu.get_barrier_semaphore()

    def greet(t, p):
        pl.semaphore_signal(barrier, inc=1, device_id=(t, p), device_id_type=MESH)

    def fellow(k):
        return upper * half_axis + (me + k) % half_axis

    def greet_upper():
        for p in range(half_axis, n_paths):
            greet(tm, p)

    pl.when(upper == 1)(lambda: greet(tm, gate))
    pl.when(upper == 0)(greet_upper)
    for k in range(1, half_axis):
        pl.when(fellow(k) != gate)(lambda: greet(tm, fellow(k)))

    def greet_across():
        for k in bits:
            greet(across(k), me)

    pl.when(upper == 0)(greet_across)


    def load(c):
        days = pl.ds(c * (steps // PIECES), steps // PIECES)
        return pltpu.make_async_copy(ret_hbm.at[days], ret.at[days], load_sem.at[c])

    for c in range(PIECES):
        load(c).start(priority=1)

    own.wait()
    pair_w[...] = jnp.concatenate([own_w[0 : share // 2], own_w[share // 2 :]], axis=1)
    wbuf[me] = pair_w[...]
    pl.when(me != gate)(lambda: pl.semaphore_wait(barrier, half_axis - 1 + len(bits) * (1 - upper) + half_axis * upper))

    def open_gate():
        pl.semaphore_signal(opened, inc=1, device_id=(tm, gate), device_id_type=MESH)

    pl.when(jnp.logical_and(upper == 0, me != gate))(open_gate)
    pl.when(me == gate)(lambda: pl.semaphore_wait(opened, half_axis - 1))

    def weights_copy(source, rows, target, sems):
        return pltpu.make_async_remote_copy(
            src_ref=source,
            dst_ref=wbuf.at[rows],
            send_sem=sems[0],
            recv_sem=sems[1],
            device_id=(tm, target),
            device_id_type=MESH,
        )

    def weights_wait(count, sems):
        rows = pl.ds(0, count)
        return weights_copy(wbuf.at[rows], rows, gate, sems)

    near_sems = near_sem, near_recv_sem

    def far_sems(p):
        return far_sem.at[p], far_recv_sem

    def send_down(act):
        def down():
            for p in range(half_axis):
                act(weights_copy(pair_w, me, p, far_sems(p)))

        pl.when(upper == 1)(down)

    def send_near(act):
        for k in range(half_axis - 1, 0, -1):
            act(weights_copy(pair_w, me, fellow(k), near_sems))

    def send_over(act):
        rows = pl.ds(0, half_axis)

        def over():
            for p in range(half_axis - 1, -1, -1):
                act(weights_copy(wbuf.at[rows], rows, half_axis + p, far_sems(p)))

        pl.when(me == gate)(over)

    send_down(lambda copy: copy.start())
    send_near(lambda copy: copy.start())
    pl.when(me == gate)(lambda: pl.semaphore_wait(barrier, half_axis + len(bits)))

    def tell(p):
        for k in (k for k in others if k.bit_count() == p):
            pl.semaphore_signal(told.at[k - 1], inc=1, device_id=(across(k & -k), me), device_id_type=MESH)

    def hear(p):
        for k in (k for k in others if k.bit_count() == p):
            pl.semaphore_wait(told.at[k - 1], 1)

    pl.when(me == gate)(lambda: tell(1))
    pl.when(me < gate)(lambda: tell(2))

    def near_arrival():
        weights_wait(half_axis - 1, near_sems).wait_recv()

    pl.when(me == gate)(near_arrival)
    send_over(lambda copy: copy.start())

    def loud_copy(k, source, slot):
        return pltpu.make_async_remote_copy(
            src_ref=source,
            dst_ref=louds.at[slot],
            send_sem=lsend_sem,
            recv_sem=lrecv_sem,
            device_id=(across(k), me),
            device_id_type=MESH,
        )

    top = jnp.zeros((LOUD, assets), ret.dtype)
    for c in range(PIECES):
        load(c).wait()

        def look(i, top):
            t, r = c * (steps // PIECES) + i // (paths // (4 * LOUD)), i % (paths // (4 * LOUD)) * (4 * LOUD)
            for q in range(4):
                top = jnp.maximum(top, jnp.abs(ret[t, pl.ds(r + q * LOUD, LOUD)]))
            return top

        top = lax.fori_loop(0, steps // PIECES * (paths // (4 * LOUD)), look, top)
    loud[...] = jnp.full(loud.shape, jnp.max(top.astype(jnp.float32)), jnp.float32)
    louds[tm] = loud[...]
    pl.when(me != gate)(near_arrival)

    def gates():
        hear(1)
        tell(2)

    pl.when(me == gate)(gates)

    def side(h):
        held = wbuf[pl.ds(h * half_axis, half_axis)]
        swap = jnp.concatenate([held[:, :, ports:], held[:, :, :ports]], axis=2)
        rows = jnp.concatenate([held[:, None], swap[:, None]], axis=1).reshape(depth, 2 * ports)
        spare = jnp.concatenate([swap[:, None], held[:, None]], axis=1).reshape(depth, 2 * ports)
        left = lax.broadcasted_iota(jnp.int32, rows.shape, 1) < ports
        blank = jnp.zeros_like(rows)
        return jnp.concatenate([jnp.where(left, rows, blank), jnp.where(left, blank, spare)], axis=0)

    def product(c, i, h, both):
        cols = pl.ds(pl.multiple_of(h * depth, depth), depth)
        first = ret[:, pl.ds(c * width + i * ROWS, ROWS), cols].reshape(steps * ROWS, depth)
        second = ret[:, pl.ds(c * width + half + i * ROWS, ROWS), cols].reshape(steps * ROWS, depth)
        return jnp.dot(
            jnp.concatenate([first, second], axis=1), both, preferred_element_type=jnp.float32
        ).reshape(steps, ROWS, 2 * ports)

    def block_copy(c, k, target, slot, first, count):
        figures = pl.ds(first, count)
        return pltpu.make_async_remote_copy(
            src_ref=send.at[c, target, figures],
            dst_ref=recv.at[c, slot, figures],
            send_sem=send_sem,
            recv_sem=recv_sem.at[c, k - 1] if isinstance(c, int) else recv_sem.at[0, 0],
            device_id=(across(k), me),
            device_id_type=MESH,
        )

    def by_segment(s, act):
        pl.when(s == 0)(lambda: act(END, 2))
        pl.when(s == n_tm - 1)(lambda: act(FALL, 2))
        pl.when(jnp.logical_and(s > 0, s < n_tm - 1))(lambda: act(END, 4))

    def send_blocks(c, act, late):
        def blocks(first, count):
            for k in others:
                if k.bit_count() > 1:
                    pl.when((across(k) > 0) == late)(lambda: act(block_copy(c, k, across(k), tm, first, count)))
                elif not late:
                    act(block_copy(c, k, across(k), tm, first, count))

        by_segment(tm, blocks)

    def block_arrival(c, k):
        s = across(k)
        by_segment(s, lambda first, count: block_copy(c, k, s, s, first, count).wait_recv())

    both = side(upper)
    for c in range(CHUNKS):
        for i in range(subs):
            part[c, i] = product(c, i, upper, both)

    def spread():
        for p in range(2, len(bits) + 1):
            hear(p)
            tell(p + 1)

    def admit():
        for p in range(half_axis, n_paths):
            pl.semaphore_signal(told.at[0], inc=1, device_id=(tm, p), device_id_type=MESH)

    pl.when(upper == 0)(spread)
    pl.when(me == gate)(admit)
    pl.when(upper == 1)(lambda: pl.semaphore_wait(told.at[0], 1))
    for k in others:
        loud_copy(k, loud, tm).start()

    weights_wait(half_axis, far_sems(0)).wait_recv()
    both = side(1 - upper)
    for c in range(CHUNKS):
        for i in range(subs):
            more[c, i] = product(c, i, 1 - upper, both)
        if c == 0:
            heavy = jnp.max(jnp.abs(wbuf[...].astype(jnp.float32))) * (assets * steps)
        scale = TOP / jnp.maximum(loud[0:1] * heavy, TINY)
        pieces = []
        for i in range(subs):
            zero = jnp.zeros((ROWS, 2 * ports), jnp.float32)
            end, fall, dip, loss = zero, zero, zero, zero
            for t in range(steps):
                gain = part[c, i, t] + more[c, i, t]
                end = jnp.maximum(end - gain, 0.0)
                fall = jnp.maximum(fall, end)
                loss = loss - gain
                dip = jnp.maximum(dip, loss)
            figures = []
            for k, figure in enumerate((end, fall, dip, loss)):
                code = figure * scale
                code = code * code
                code = code * code
                code = code * code
                if k == LOSS:
                    code = jnp.where(figure < 0, -code, code)
                figures.append(code.astype(jnp.bfloat16))
            pieces.append(figures)
        for k in range(4):
            whole = jnp.concatenate([piece[k] for piece in pieces], axis=0).T
            for b in range(n_tm):
                rows = b * block
                send[c, b, k, :, 0:half] = whole[rows : rows + block]
                send[c, b, k, :, half:width] = whole[ports + rows : ports + rows + block]
        send_blocks(c, lambda copy: copy.start(), False)

    for c in range(CHUNKS):
        send_blocks(c, lambda copy: copy.start(), True)
    send_down(lambda copy: copy.wait_send())
    weights_wait(half_axis - 1, near_sems).wait_send()
    send_over(lambda copy: copy.wait_send())
    rest = pl.ds(0, n_tm - 1)
    loud_copy(1, louds.at[rest], rest).wait_send()
    loud_copy(1, louds.at[rest], rest).wait_recv()

    def decode(codes, s):
        unit = jnp.maximum(louds[s, 0:1] * heavy, TINY) / TOP
        unit = jnp.concatenate([unit] * (width // unit.shape[1]), axis=1)
        code = codes.astype(jnp.float32)
        size = jnp.exp(jnp.log(jnp.abs(code)) * 0.125) * unit[None]
        values[s] = jnp.concatenate([size[:LOSS], jnp.where(code[LOSS:] < 0, -size[LOSS:], size[LOSS:])], axis=0)

    def drain(first, count):
        block_copy(pl.ds(0, CHUNKS), 1, rest, rest, first, count).wait_send()

    for c in range(CHUNKS):
        decode(send[c, tm], tm)
        for k in arrivals:
            if (c, k) == (CHUNKS - 1, arrivals[-1]):
                by_segment(tm, drain)
            block_arrival(c, k)
            decode(recv[c, across(k)], across(k))
        end, fall = values[0, END], values[0, FALL]
        for s in range(1, n_tm):
            fall = jnp.maximum(jnp.maximum(fall, values[s, FALL]), end + values[s, DIP])
            if s < n_tm - 1:
                end = jnp.maximum(end + values[s, LOSS], values[s, END])
        out_ref[:, pl.ds(c * width, width)] = fall


def solution(mesh):
    n_tm, n_paths = mesh.shape["tm"], mesh.shape["paths"]

    def shards(returns, weights):
        steps, paths, assets = returns.shape
        share, ports = weights.shape
        block, width = ports // n_tm, paths // CHUNKS
        subs = width // 2 // ROWS
        dma = pltpu.SemaphoreType.DMA
        return pl.pallas_call(
            functools.partial(kernel, n_tm, n_paths),
            out_shape=jax.ShapeDtypeStruct((block, paths), jnp.float32),
            in_specs=[
                pl.BlockSpec(memory_space=pltpu.HBM),
                pl.BlockSpec(memory_space=pltpu.HBM),
            ],
            out_specs=pl.BlockSpec(memory_space=pltpu.VMEM),
            scratch_shapes=[
                pltpu.VMEM((steps, paths, assets), returns.dtype),
                pltpu.VMEM((share, ports), weights.dtype),
                pltpu.VMEM((share // 2, 2 * ports), weights.dtype),
                pltpu.VMEM((n_paths, share // 2, 2 * ports), weights.dtype),
                pltpu.VMEM((CHUNKS, subs, steps, ROWS, 2 * ports), jnp.float32),
                pltpu.VMEM((CHUNKS, subs, steps, ROWS, 2 * ports), jnp.float32),
                pltpu.VMEM((CHUNKS, n_tm, 4, block, width), jnp.bfloat16),
                pltpu.VMEM((CHUNKS, n_tm, 4, block, width), jnp.bfloat16),
                pltpu.VMEM((8, 2 * ports), jnp.float32),
                pltpu.VMEM((n_tm, 8, 2 * ports), jnp.float32),
                pltpu.VMEM((n_tm, 4, block, width), jnp.float32),
                dma((PIECES,)),
                dma,
                pltpu.SemaphoreType.REGULAR((n_tm - 1,)),
                pltpu.SemaphoreType.REGULAR,
                dma,
                dma,
                dma((n_paths // 2,)),
                dma,
                dma,
                dma((CHUNKS, n_tm - 1)),
                dma,
                dma,
            ],
            compiler_params=pltpu.CompilerParams(
                collective_id=0, has_side_effects=True, vmem_limit_bytes=32 << 20
            ),
        )(
            pltpu.with_memory_space_constraint(returns, pltpu.HBM),
            pltpu.with_memory_space_constraint(weights, pltpu.HBM),
        )

    in_specs = (P("tm", "paths", None), P("paths", None))
    out_specs = P("tm", "paths")
    return jax.shard_map(shards, mesh=mesh, in_specs=in_specs, out_specs=out_specs, check_vma=False)
```

```python
import functools

import jax
import jax.numpy as jnp
from jax import lax
from jax.experimental import pallas as pl
from jax.experimental.pallas import tpu as pltpu
from jax.sharding import PartitionSpec as P

MESH = pl.DeviceIdType.MESH
CHUNKS = 2
ROWS = 32
PIECES = 4
LOUD = 64
END, FALL, DIP, LOSS = range(4)
TOP = 2.0**15.75
TINY = 1e-30


def kernel(
    n_tm, n_paths, ret_hbm, w_hbm, out_ref,
    ret, own_w, pair_w, wbuf, wraw, part, more, send, recv, loud, louds, values,
    load_sem, own_sem, told, opened, near_sem, near_recv_sem, far_sem, far_recv_sem, send_sem, recv_sem, lsend_sem, lrecv_sem,
):
    steps, paths, assets = ret.shape
    ports = own_w.shape[1]
    block = ports // n_tm
    width = paths // CHUNKS
    half = width // 2
    depth = assets // 2
    subs = half // ROWS
    tm = lax.axis_index("tm")
    me = lax.axis_index("paths")
    share = own_w.shape[0]

    own = pltpu.make_async_copy(w_hbm, own_w, own_sem)
    own.start()
    bits = [1 << i for i in range(n_tm.bit_length() - 1)]
    others = sorted(range(1, n_tm), key=lambda k: -k.bit_count())
    arrivals = others[::-1]

    def across(k):
        other = tm
        for bit in (b for b in bits if b & k):
            other = other + bit - 2 * bit * ((tm // bit) % 2)
        return other

    half_axis = n_paths // 2
    upper = me // half_axis
    gate = half_axis - 1
    barrier = pltpu.get_barrier_semaphore()

    def greet(t, p):
        pl.semaphore_signal(barrier, inc=1, device_id=(t, p), device_id_type=MESH)

    def fellow(k):
        return upper * half_axis + (me + k) % half_axis

    def greet_upper():
        for p in range(half_axis, n_paths):
            greet(tm, p)

    pl.when(upper == 1)(lambda: greet(tm, gate))
    pl.when(upper == 0)(greet_upper)
    for k in range(1, half_axis):
        pl.when(fellow(k) != gate)(lambda: greet(tm, fellow(k)))

    def greet_across():
        for k in bits:
            greet(across(k), me)

    pl.when(upper == 0)(greet_across)


    def load(c):
        days = pl.ds(c * (steps // PIECES), steps // PIECES)
        return pltpu.make_async_copy(ret_hbm.at[days], ret.at[days], load_sem.at[c])

    for c in range(PIECES):
        load(c).start(priority=1)

    pl.when(me != gate)(lambda: pl.semaphore_wait(barrier, half_axis - 1 + len(bits) * (1 - upper) + half_axis * upper))

    def open_gate():
        pl.semaphore_signal(opened, inc=1, device_id=(tm, gate), device_id_type=MESH)

    pl.when(jnp.logical_and(upper == 0, me != gate))(open_gate)
    pl.when(me == gate)(lambda: pl.semaphore_wait(opened, half_axis - 1))

    own.wait()
    def weights_copy(source, rows, target, sems):
        return pltpu.make_async_remote_copy(
            src_ref=source,
            dst_ref=wbuf.at[rows],
            send_sem=sems[0],
            recv_sem=sems[1],
            device_id=(tm, target),
            device_id_type=MESH,
        )

    def weights_wait(count, sems):
        rows = pl.ds(0, count)
        return weights_copy(wbuf.at[rows], rows, gate, sems)

    near_sems = near_sem, near_recv_sem

    def far_sems(p):
        return far_sem.at[p], far_recv_sem

    def raw_copy(source, rows, p):
        return pltpu.make_async_remote_copy(
            src_ref=source,
            dst_ref=wraw.at[rows],
            send_sem=far_sem.at[p],
            recv_sem=far_recv_sem,
            device_id=(tm, p),
            device_id_type=MESH,
        )

    def send_down(act):
        def down():
            for p in range(half_axis):
                act(raw_copy(own_w, me - half_axis, p))

        pl.when(upper == 1)(down)

    def send_near(act):
        for k in range(half_axis - 1, 0, -1):
            act(weights_copy(pair_w, me, fellow(k), near_sems))

    def send_over(act):
        rows = pl.ds(0, half_axis)

        def over():
            for p in range(half_axis - 1, -1, -1):
                act(weights_copy(wbuf.at[rows], rows, half_axis + p, far_sems(p)))

        pl.when(me == gate)(over)

    send_down(lambda copy: copy.start())
    pair_w[...] = jnp.concatenate([own_w[0 : share // 2], own_w[share // 2 :]], axis=1)
    wbuf[me] = pair_w[...]
    send_near(lambda copy: copy.start())
    pl.when(me == gate)(lambda: pl.semaphore_wait(barrier, half_axis + len(bits)))

    def tell(p):
        for k in (k for k in others if k.bit_count() == p):
            pl.semaphore_signal(told.at[k - 1], inc=1, device_id=(across(k & -k), me), device_id_type=MESH)

    def hear(p):
        for k in (k for k in others if k.bit_count() == p):
            pl.semaphore_wait(told.at[k - 1], 1)

    pl.when(me == gate)(lambda: tell(1))
    pl.when(me < gate)(lambda: tell(2))

    def near_arrival():
        weights_wait(half_axis - 1, near_sems).wait_recv()

    pl.when(me == gate)(near_arrival)
    send_over(lambda copy: copy.start())

    def loud_copy(k, source, slot):
        return pltpu.make_async_remote_copy(
            src_ref=source,
            dst_ref=louds.at[slot],
            send_sem=lsend_sem,
            recv_sem=lrecv_sem,
            device_id=(across(k), me),
            device_id_type=MESH,
        )

    top = jnp.zeros((LOUD, assets), ret.dtype)
    for c in range(PIECES):
        load(c).wait()

        def look(i, top):
            t, r = c * (steps // PIECES) + i // (paths // (4 * LOUD)), i % (paths // (4 * LOUD)) * (4 * LOUD)
            for q in range(4):
                top = jnp.maximum(top, jnp.abs(ret[t, pl.ds(r + q * LOUD, LOUD)]))
            return top

        top = lax.fori_loop(0, steps // PIECES * (paths // (4 * LOUD)), look, top)
    loud[...] = jnp.full(loud.shape, jnp.max(top.astype(jnp.float32)), jnp.float32)
    louds[tm] = loud[...]
    pl.when(me != gate)(near_arrival)

    def gates():
        hear(1)
        tell(2)

    pl.when(me == gate)(gates)

    def side(h):
        held = wbuf[pl.ds(h * half_axis, half_axis)]
        swap = jnp.concatenate([held[:, :, ports:], held[:, :, :ports]], axis=2)
        rows = jnp.concatenate([held[:, None], swap[:, None]], axis=1).reshape(depth, 2 * ports)
        spare = jnp.concatenate([swap[:, None], held[:, None]], axis=1).reshape(depth, 2 * ports)
        left = lax.broadcasted_iota(jnp.int32, rows.shape, 1) < ports
        blank = jnp.zeros_like(rows)
        return jnp.concatenate([jnp.where(left, rows, blank), jnp.where(left, blank, spare)], axis=0)

    def product(c, i, h, both):
        cols = pl.ds(pl.multiple_of(h * depth, depth), depth)
        first = ret[:, pl.ds(c * width + i * ROWS, ROWS), cols].reshape(steps * ROWS, depth)
        second = ret[:, pl.ds(c * width + half + i * ROWS, ROWS), cols].reshape(steps * ROWS, depth)
        return jnp.dot(
            jnp.concatenate([first, second], axis=1), both, preferred_element_type=jnp.float32
        ).reshape(steps, ROWS, 2 * ports)

    def block_copy(c, k, target, slot, first, count):
        figures = pl.ds(first, count)
        return pltpu.make_async_remote_copy(
            src_ref=send.at[c, target, figures],
            dst_ref=recv.at[c, slot, figures],
            send_sem=send_sem,
            recv_sem=recv_sem.at[c, k - 1] if isinstance(c, int) else recv_sem.at[0, 0],
            device_id=(across(k), me),
            device_id_type=MESH,
        )

    def by_segment(s, act):
        pl.when(s == 0)(lambda: act(END, 2))
        pl.when(s == n_tm - 1)(lambda: act(FALL, 2))
        pl.when(jnp.logical_and(s > 0, s < n_tm - 1))(lambda: act(END, 4))

    def send_blocks(c, act, late):
        def blocks(first, count):
            for k in others:
                if k.bit_count() > 1:
                    pl.when((across(k) > 0) == late)(lambda: act(block_copy(c, k, across(k), tm, first, count)))
                elif not late:
                    act(block_copy(c, k, across(k), tm, first, count))

        by_segment(tm, blocks)

    def block_arrival(c, k):
        s = across(k)
        by_segment(s, lambda first, count: block_copy(c, k, s, s, first, count).wait_recv())

    both = side(upper)
    for c in range(CHUNKS):
        for i in range(subs):
            part[c, i] = product(c, i, upper, both)

    def spread():
        for p in range(2, len(bits) + 1):
            hear(p)
            tell(p + 1)

    def admit():
        for p in range(half_axis, n_paths):
            pl.semaphore_signal(told.at[0], inc=1, device_id=(tm, p), device_id_type=MESH)

    pl.when(upper == 0)(spread)
    pl.when(me == gate)(admit)
    pl.when(upper == 1)(lambda: pl.semaphore_wait(told.at[0], 1))
    for k in others:
        loud_copy(k, loud, tm).start()

    rows = pl.ds(0, half_axis)
    pl.when(upper == 1)(lambda: weights_wait(half_axis, far_sems(0)).wait_recv())
    pl.when(upper == 0)(lambda: raw_copy(wraw.at[rows], rows, 0).wait_recv())
    raw = wraw[...].reshape(depth, ports)
    blank = jnp.zeros_like(raw)
    low = jnp.concatenate(
        [jnp.concatenate([raw, blank], axis=1), jnp.concatenate([blank, raw], axis=1)], axis=0
    )
    near_top = jnp.max(jnp.abs(both.astype(jnp.float32)))
    both = jnp.where(upper == 1, side(0), low)
    for c in range(CHUNKS):
        for i in range(subs):
            more[c, i] = product(c, i, 1 - upper, both)
        if c == 0:
            heavy = jnp.maximum(near_top, jnp.max(jnp.abs(both.astype(jnp.float32)))) * (assets * steps)
        scale = TOP / jnp.maximum(loud[0:1] * heavy, TINY)
        pieces = []
        for i in range(subs):
            zero = jnp.zeros((ROWS, 2 * ports), jnp.float32)
            end, fall, dip, loss = zero, zero, zero, zero
            for t in range(steps):
                gain = part[c, i, t] + more[c, i, t]
                end = jnp.maximum(end - gain, 0.0)
                fall = jnp.maximum(fall, end)
                loss = loss - gain
                dip = jnp.maximum(dip, loss)
            figures = []
            for k, figure in enumerate((end, fall, dip, loss)):
                code = figure * scale
                code = code * code
                code = code * code
                code = code * code
                if k == LOSS:
                    code = jnp.where(figure < 0, -code, code)
                figures.append(code.astype(jnp.bfloat16))
            pieces.append(figures)
        for k in range(4):
            whole = jnp.concatenate([piece[k] for piece in pieces], axis=0).T
            for b in range(n_tm):
                rows = b * block
                send[c, b, k, :, 0:half] = whole[rows : rows + block]
                send[c, b, k, :, half:width] = whole[ports + rows : ports + rows + block]
        send_blocks(c, lambda copy: copy.start(), False)

    for c in range(CHUNKS):
        send_blocks(c, lambda copy: copy.start(), True)
    send_down(lambda copy: copy.wait_send())
    weights_wait(half_axis - 1, near_sems).wait_send()
    send_over(lambda copy: copy.wait_send())
    rest = pl.ds(0, n_tm - 1)
    loud_copy(1, louds.at[rest], rest).wait_send()
    loud_copy(1, louds.at[rest], rest).wait_recv()

    def decode(codes, s):
        unit = jnp.maximum(louds[s, 0:1] * heavy, TINY) / TOP
        unit = jnp.concatenate([unit] * (width // unit.shape[1]), axis=1)
        code = codes.astype(jnp.float32)
        size = jnp.exp(jnp.log(jnp.abs(code)) * 0.125) * unit[None]
        values[s] = jnp.concatenate([size[:LOSS], jnp.where(code[LOSS:] < 0, -size[LOSS:], size[LOSS:])], axis=0)

    def drain(first, count):
        block_copy(pl.ds(0, CHUNKS), 1, rest, rest, first, count).wait_send()

    for c in range(CHUNKS):
        decode(send[c, tm], tm)
        for k in arrivals:
            if (c, k) == (CHUNKS - 1, arrivals[-1]):
                by_segment(tm, drain)
            block_arrival(c, k)
            decode(recv[c, across(k)], across(k))
        end, fall = values[0, END], values[0, FALL]
        for s in range(1, n_tm):
            fall = jnp.maximum(jnp.maximum(fall, values[s, FALL]), end + values[s, DIP])
            if s < n_tm - 1:
                end = jnp.maximum(end + values[s, LOSS], values[s, END])
        out_ref[:, pl.ds(c * width, width)] = fall


def solution(mesh):
    n_tm, n_paths = mesh.shape["tm"], mesh.shape["paths"]

    def shards(returns, weights):
        steps, paths, assets = returns.shape
        share, ports = weights.shape
        block, width = ports // n_tm, paths // CHUNKS
        subs = width // 2 // ROWS
        dma = pltpu.SemaphoreType.DMA
        return pl.pallas_call(
            functools.partial(kernel, n_tm, n_paths),
            out_shape=jax.ShapeDtypeStruct((block, paths), jnp.float32),
            in_specs=[
                pl.BlockSpec(memory_space=pltpu.HBM),
                pl.BlockSpec(memory_space=pltpu.HBM),
            ],
            out_specs=pl.BlockSpec(memory_space=pltpu.VMEM),
            scratch_shapes=[
                pltpu.VMEM((steps, paths, assets), returns.dtype),
                pltpu.VMEM((share, ports), weights.dtype),
                pltpu.VMEM((share // 2, 2 * ports), weights.dtype),
                pltpu.VMEM((n_paths, share // 2, 2 * ports), weights.dtype),
                pltpu.VMEM((n_paths // 2, share, ports), weights.dtype),
                pltpu.VMEM((CHUNKS, subs, steps, ROWS, 2 * ports), jnp.float32),
                pltpu.VMEM((CHUNKS, subs, steps, ROWS, 2 * ports), jnp.float32),
                pltpu.VMEM((CHUNKS, n_tm, 4, block, width), jnp.bfloat16),
                pltpu.VMEM((CHUNKS, n_tm, 4, block, width), jnp.bfloat16),
                pltpu.VMEM((8, 2 * ports), jnp.float32),
                pltpu.VMEM((n_tm, 8, 2 * ports), jnp.float32),
                pltpu.VMEM((n_tm, 4, block, width), jnp.float32),
                dma((PIECES,)),
                dma,
                pltpu.SemaphoreType.REGULAR((n_tm - 1,)),
                pltpu.SemaphoreType.REGULAR,
                dma,
                dma,
                dma((n_paths // 2,)),
                dma,
                dma,
                dma((CHUNKS, n_tm - 1)),
                dma,
                dma,
            ],
            compiler_params=pltpu.CompilerParams(
                collective_id=0, has_side_effects=True, vmem_limit_bytes=32 << 20
            ),
        )(
            pltpu.with_memory_space_constraint(returns, pltpu.HBM),
            pltpu.with_memory_space_constraint(weights, pltpu.HBM),
        )

    in_specs = (P("tm", "paths", None), P("paths", None))
    out_specs = P("tm", "paths")
    return jax.shard_map(shards, mesh=mesh, in_specs=in_specs, out_specs=out_specs, check_vma=False)
```

```python
import functools

import jax
import jax.numpy as jnp
from jax import lax
from jax.experimental import pallas as pl
from jax.experimental.pallas import tpu as pltpu
from jax.sharding import PartitionSpec as P

MESH = pl.DeviceIdType.MESH
CHUNKS = 2
ROWS = 16
PIECES = 4
LOUD = 64
END, FALL, DIP, LOSS = range(4)
TOP = 2.0**15.75
TINY = 1e-30


def kernel(
    n_tm, n_paths, ret_hbm, w_hbm, out_ref,
    ret, own_w, pair_w, wbuf, wraw, part, more, send, recv, loud, louds, values,
    load_sem, own_sem, told, opened, near_sem, near_recv_sem, far_sem, far_recv_sem, send_sem, recv_sem, lsend_sem, lrecv_sem,
):
    steps, paths, assets = ret.shape
    ports = own_w.shape[1]
    block = ports // n_tm
    width = paths // CHUNKS
    half = width // 2
    depth = assets // 2
    subs = half // ROWS
    tm = lax.axis_index("tm")
    me = lax.axis_index("paths")
    share = own_w.shape[0]

    own = pltpu.make_async_copy(w_hbm, own_w, own_sem)
    own.start()
    bits = [1 << i for i in range(n_tm.bit_length() - 1)]
    others = sorted(range(1, n_tm), key=lambda k: -k.bit_count())
    arrivals = others[::-1]

    def across(k):
        other = tm
        for bit in (b for b in bits if b & k):
            other = other + bit - 2 * bit * ((tm // bit) % 2)
        return other

    half_axis = n_paths // 2
    upper = me // half_axis
    gate = half_axis - 1
    barrier = pltpu.get_barrier_semaphore()

    def greet(t, p):
        pl.semaphore_signal(barrier, inc=1, device_id=(t, p), device_id_type=MESH)

    def fellow(k):
        return upper * half_axis + (me + k) % half_axis

    def greet_upper():
        for p in range(half_axis, n_paths):
            greet(tm, p)

    pl.when(upper == 1)(lambda: greet(tm, gate))
    pl.when(upper == 0)(greet_upper)
    for k in range(1, half_axis):
        pl.when(fellow(k) != gate)(lambda: greet(tm, fellow(k)))

    def greet_across():
        for k in bits:
            greet(across(k), me)

    pl.when(upper == 0)(greet_across)


    def load(c):
        days = pl.ds(c * (steps // PIECES), steps // PIECES)
        return pltpu.make_async_copy(ret_hbm.at[days], ret.at[days], load_sem.at[c])

    for c in range(PIECES):
        load(c).start(priority=1)

    pl.when(me != gate)(lambda: pl.semaphore_wait(barrier, half_axis - 1 + len(bits) * (1 - upper) + half_axis * upper))

    def open_gate():
        pl.semaphore_signal(opened, inc=1, device_id=(tm, gate), device_id_type=MESH)

    pl.when(jnp.logical_and(upper == 0, me != gate))(open_gate)
    pl.when(me == gate)(lambda: pl.semaphore_wait(opened, half_axis - 1))

    own.wait()
    def weights_copy(source, rows, target, sems):
        return pltpu.make_async_remote_copy(
            src_ref=source,
            dst_ref=wbuf.at[rows],
            send_sem=sems[0],
            recv_sem=sems[1],
            device_id=(tm, target),
            device_id_type=MESH,
        )

    def weights_wait(count, sems):
        rows = pl.ds(0, count)
        return weights_copy(wbuf.at[rows], rows, gate, sems)

    near_sems = near_sem, near_recv_sem

    def far_sems(p):
        return far_sem.at[p], far_recv_sem

    def raw_copy(source, rows, p):
        return pltpu.make_async_remote_copy(
            src_ref=source,
            dst_ref=wraw.at[rows],
            send_sem=far_sem.at[p],
            recv_sem=far_recv_sem,
            device_id=(tm, p),
            device_id_type=MESH,
        )

    def send_down(act):
        def down():
            for p in range(half_axis):
                act(raw_copy(own_w, me - half_axis, p))

        pl.when(upper == 1)(down)

    def send_near(act):
        for k in range(half_axis - 1, 0, -1):
            act(weights_copy(pair_w, me, fellow(k), near_sems))

    def send_over(act):
        rows = pl.ds(0, half_axis)

        def over():
            for p in range(half_axis - 1, -1, -1):
                act(weights_copy(wbuf.at[rows], rows, half_axis + p, far_sems(p)))

        pl.when(me == gate)(over)

    send_down(lambda copy: copy.start())
    pair_w[...] = jnp.concatenate([own_w[0 : share // 2], own_w[share // 2 :]], axis=1)
    wbuf[me] = pair_w[...]
    send_near(lambda copy: copy.start())
    pl.when(me == gate)(lambda: pl.semaphore_wait(barrier, half_axis + len(bits)))

    def tell(p):
        for k in (k for k in others if k.bit_count() == p):
            pl.semaphore_signal(told.at[k - 1], inc=1, device_id=(across(k & -k), me), device_id_type=MESH)

    def hear(p):
        for k in (k for k in others if k.bit_count() == p):
            pl.semaphore_wait(told.at[k - 1], 1)

    pl.when(me == gate)(lambda: tell(1))
    pl.when(me < gate)(lambda: tell(2))

    def near_arrival():
        weights_wait(half_axis - 1, near_sems).wait_recv()

    pl.when(me == gate)(near_arrival)
    send_over(lambda copy: copy.start())

    def loud_copy(k, source, slot):
        return pltpu.make_async_remote_copy(
            src_ref=source,
            dst_ref=louds.at[slot],
            send_sem=lsend_sem,
            recv_sem=lrecv_sem,
            device_id=(across(k), me),
            device_id_type=MESH,
        )

    top = jnp.zeros((LOUD, assets), ret.dtype)
    for c in range(PIECES):
        load(c).wait()

        def look(i, top):
            t, r = c * (steps // PIECES) + i // (paths // (4 * LOUD)), i % (paths // (4 * LOUD)) * (4 * LOUD)
            for q in range(4):
                top = jnp.maximum(top, jnp.abs(ret[t, pl.ds(r + q * LOUD, LOUD)]))
            return top

        top = lax.fori_loop(0, steps // PIECES * (paths // (4 * LOUD)), look, top)
    loud[...] = jnp.full(loud.shape, jnp.max(top.astype(jnp.float32)), jnp.float32)
    louds[tm] = loud[...]
    pl.when(me != gate)(near_arrival)

    def gates():
        hear(1)
        tell(2)

    pl.when(me == gate)(gates)

    def side(h):
        held = wbuf[pl.ds(h * half_axis, half_axis)]
        swap = jnp.concatenate([held[:, :, ports:], held[:, :, :ports]], axis=2)
        rows = jnp.concatenate([held[:, None], swap[:, None]], axis=1).reshape(depth, 2 * ports)
        spare = jnp.concatenate([swap[:, None], held[:, None]], axis=1).reshape(depth, 2 * ports)
        left = lax.broadcasted_iota(jnp.int32, rows.shape, 1) < ports
        blank = jnp.zeros_like(rows)
        return jnp.concatenate([jnp.where(left, rows, blank), jnp.where(left, blank, spare)], axis=0)

    def product(c, i, h, both):
        cols = pl.ds(pl.multiple_of(h * depth, depth), depth)
        first = ret[:, pl.ds(c * width + i * ROWS, ROWS), cols].reshape(steps * ROWS, depth)
        second = ret[:, pl.ds(c * width + half + i * ROWS, ROWS), cols].reshape(steps * ROWS, depth)
        return jnp.dot(
            jnp.concatenate([first, second], axis=1), both, preferred_element_type=jnp.float32
        ).reshape(steps, ROWS, 2 * ports)

    def block_copy(c, k, target, slot, first, count):
        figures = pl.ds(first, count)
        return pltpu.make_async_remote_copy(
            src_ref=send.at[c, target, figures],
            dst_ref=recv.at[c, slot, figures],
            send_sem=send_sem,
            recv_sem=recv_sem.at[c, k - 1] if isinstance(c, int) else recv_sem.at[0, 0],
            device_id=(across(k), me),
            device_id_type=MESH,
        )

    def by_segment(s, act):
        pl.when(s == 0)(lambda: act(END, 2))
        pl.when(s == n_tm - 1)(lambda: act(FALL, 2))
        pl.when(jnp.logical_and(s > 0, s < n_tm - 1))(lambda: act(END, 4))

    def send_blocks(c, act, late):
        def blocks(first, count):
            for k in others:
                if k.bit_count() > 1:
                    pl.when((across(k) > 0) == late)(lambda: act(block_copy(c, k, across(k), tm, first, count)))
                elif not late:
                    act(block_copy(c, k, across(k), tm, first, count))

        by_segment(tm, blocks)

    def block_arrival(c, k):
        s = across(k)
        by_segment(s, lambda first, count: block_copy(c, k, s, s, first, count).wait_recv())

    both = side(upper)
    for c in range(CHUNKS):
        for i in range(subs):
            part[c, i] = product(c, i, upper, both)

    def spread():
        for p in range(2, len(bits) + 1):
            hear(p)
            tell(p + 1)

    def admit():
        for p in range(half_axis, n_paths):
            pl.semaphore_signal(told.at[0], inc=1, device_id=(tm, p), device_id_type=MESH)

    pl.when(upper == 0)(spread)
    pl.when(me == gate)(admit)
    pl.when(upper == 1)(lambda: pl.semaphore_wait(told.at[0], 1))
    for k in others:
        loud_copy(k, loud, tm).start()

    rows = pl.ds(0, half_axis)
    pl.when(upper == 1)(lambda: weights_wait(half_axis, far_sems(0)).wait_recv())
    pl.when(upper == 0)(lambda: raw_copy(wraw.at[rows], rows, 0).wait_recv())
    raw = wraw[...].reshape(depth, ports)
    blank = jnp.zeros_like(raw)
    low = jnp.concatenate(
        [jnp.concatenate([raw, blank], axis=1), jnp.concatenate([blank, raw], axis=1)], axis=0
    )
    near_top = jnp.max(jnp.abs(both.astype(jnp.float32)))
    both = jnp.where(upper == 1, side(0), low)
    for c in range(CHUNKS):
        for i in range(subs):
            more[c, i] = product(c, i, 1 - upper, both)
        if c == 0:
            heavy = jnp.maximum(near_top, jnp.max(jnp.abs(both.astype(jnp.float32)))) * (assets * steps)
        scale = TOP / jnp.maximum(loud[0:1] * heavy, TINY)
        pieces = []
        for i in range(subs):
            zero = jnp.zeros((ROWS, 2 * ports), jnp.float32)
            end, fall, dip, loss = zero, zero, zero, zero
            for t in range(steps):
                gain = part[c, i, t] + more[c, i, t]
                end = jnp.maximum(end - gain, 0.0)
                fall = jnp.maximum(fall, end)
                loss = loss - gain
                dip = jnp.maximum(dip, loss)
            figures = []
            for k, figure in enumerate((end, fall, dip, loss)):
                code = figure * scale
                code = code * code
                code = code * code
                code = code * code
                if k == LOSS:
                    code = jnp.where(figure < 0, -code, code)
                figures.append(code.astype(jnp.bfloat16))
            pieces.append(figures)
        for k in range(4):
            whole = jnp.concatenate([piece[k] for piece in pieces], axis=0).T
            for b in range(n_tm):
                rows = b * block
                send[c, b, k, :, 0:half] = whole[rows : rows + block]
                send[c, b, k, :, half:width] = whole[ports + rows : ports + rows + block]
        send_blocks(c, lambda copy: copy.start(), False)

    for c in range(CHUNKS):
        send_blocks(c, lambda copy: copy.start(), True)
    send_down(lambda copy: copy.wait_send())
    weights_wait(half_axis - 1, near_sems).wait_send()
    send_over(lambda copy: copy.wait_send())
    rest = pl.ds(0, n_tm - 1)
    loud_copy(1, louds.at[rest], rest).wait_send()
    loud_copy(1, louds.at[rest], rest).wait_recv()

    def decode(codes, s):
        unit = jnp.maximum(louds[s, 0:1] * heavy, TINY) / TOP
        unit = jnp.concatenate([unit] * (width // unit.shape[1]), axis=1)
        code = codes.astype(jnp.float32)
        size = jnp.exp(jnp.log(jnp.abs(code)) * 0.125) * unit[None]
        values[s] = jnp.concatenate([size[:LOSS], jnp.where(code[LOSS:] < 0, -size[LOSS:], size[LOSS:])], axis=0)

    def drain(first, count):
        block_copy(pl.ds(0, CHUNKS), 1, rest, rest, first, count).wait_send()

    for c in range(CHUNKS):
        decode(send[c, tm], tm)
        for k in arrivals:
            if (c, k) == (CHUNKS - 1, arrivals[-1]):
                by_segment(tm, drain)
            block_arrival(c, k)
            decode(recv[c, across(k)], across(k))
        end, fall = values[0, END], values[0, FALL]
        for s in range(1, n_tm):
            fall = jnp.maximum(jnp.maximum(fall, values[s, FALL]), end + values[s, DIP])
            if s < n_tm - 1:
                end = jnp.maximum(end + values[s, LOSS], values[s, END])
        out_ref[:, pl.ds(c * width, width)] = fall


def solution(mesh):
    n_tm, n_paths = mesh.shape["tm"], mesh.shape["paths"]

    def shards(returns, weights):
        steps, paths, assets = returns.shape
        share, ports = weights.shape
        block, width = ports // n_tm, paths // CHUNKS
        subs = width // 2 // ROWS
        dma = pltpu.SemaphoreType.DMA
        return pl.pallas_call(
            functools.partial(kernel, n_tm, n_paths),
            out_shape=jax.ShapeDtypeStruct((block, paths), jnp.float32),
            in_specs=[
                pl.BlockSpec(memory_space=pltpu.HBM),
                pl.BlockSpec(memory_space=pltpu.HBM),
            ],
            out_specs=pl.BlockSpec(memory_space=pltpu.VMEM),
            scratch_shapes=[
                pltpu.VMEM((steps, paths, assets), returns.dtype),
                pltpu.VMEM((share, ports), weights.dtype),
                pltpu.VMEM((share // 2, 2 * ports), weights.dtype),
                pltpu.VMEM((n_paths, share // 2, 2 * ports), weights.dtype),
                pltpu.VMEM((n_paths // 2, share, ports), weights.dtype),
                pltpu.VMEM((CHUNKS, subs, steps, ROWS, 2 * ports), jnp.float32),
                pltpu.VMEM((CHUNKS, subs, steps, ROWS, 2 * ports), jnp.float32),
                pltpu.VMEM((CHUNKS, n_tm, 4, block, width), jnp.bfloat16),
                pltpu.VMEM((CHUNKS, n_tm, 4, block, width), jnp.bfloat16),
                pltpu.VMEM((8, 2 * ports), jnp.float32),
                pltpu.VMEM((n_tm, 8, 2 * ports), jnp.float32),
                pltpu.VMEM((n_tm, 4, block, width), jnp.float32),
                dma((PIECES,)),
                dma,
                pltpu.SemaphoreType.REGULAR((n_tm - 1,)),
                pltpu.SemaphoreType.REGULAR,
                dma,
                dma,
                dma((n_paths // 2,)),
                dma,
                dma,
                dma((CHUNKS, n_tm - 1)),
                dma,
                dma,
            ],
            compiler_params=pltpu.CompilerParams(
                collective_id=0, has_side_effects=True, vmem_limit_bytes=32 << 20
            ),
        )(
            pltpu.with_memory_space_constraint(returns, pltpu.HBM),
            pltpu.with_memory_space_constraint(weights, pltpu.HBM),
        )

    in_specs = (P("tm", "paths", None), P("paths", None))
    out_specs = P("tm", "paths")
    return jax.shard_map(shards, mesh=mesh, in_specs=in_specs, out_specs=out_specs, check_vma=False)
```
